16 devices in a mesh: pod: 4 (over z, y), data: 4 (over x, core).
Axes of the slice: x: 2, y: 2, z: 2, core: 2. Of those that a mesh axis runs over, the one named last changes fastest.
Arguments:
- w_first: float32 [16, 256, 1024], replicated
- w_second: float32 [16, 1024, 256], replicated
- m_first: float32 [16, 256, 1024], replicated
- m_second: float32 [16, 1024, 256], replicated
- x_now: bfloat16 [16384, 256], P(('pod', 'data'))
- y_now: bfloat16 [16384, 256], P(('pod', 'data'))
- x_next: bfloat16 [16384, 256], P(('pod', 'data'))
- y_next: bfloat16 [16384, 256], P(('pod', 'data'))
Outputs:
- output 1: float32 [16, 256, 1024], replicated
- output 2: float32 [16, 1024, 256], replicated
- output 3: float32 [16, 256, 1024], replicated
- output 4: float32 [16, 1024, 256], replicated
- output 5: float32 [16384], P(('pod', 'data'))
- output 6: float32 [16384, 256], P(('pod', 'data'))
All inputs are finite; a program needn't handle non-finite values.
Results may differ from the reference program's by a relative error of at most 0.011314.
Values are sent between devices in bfloat16 or wider.
A program may use at most 1 GiB of HBM per device.

```python
import jax
import jax.numpy as jnp
from jax import lax

D = 256
F = 1024
LAYERS = 16
TOK = 1024
DEVICES = 16
BATCH = TOK * DEVICES
LEARN_RATE = 0.25 / LAYERS
MOMENTUM = 0.9
BRANCH_SCALE = (4.0 / max(LAYERS, 4)) ** 0.5


def draw_batch(key_list):
    noise_val = jax.random.normal(key_list[0], (DEVICES, TOK, D), jnp.float32)
    global_off = jax.random.normal(key_list[1], (1, 1, D), jnp.float32)
    device_off = jax.random.normal(key_list[2], (DEVICES, 1, D), jnp.float32)
    rows_val = 0.7 * noise_val + 0.5 * global_off + 0.5 * device_off
    return rows_val.reshape(BATCH, D).astype(jnp.bfloat16)


def setup_inputs(seed: int = 0) -> dict:
    key_list = jax.random.split(jax.random.key(seed), 16)
    w_first = jax.random.normal(key_list[0], (LAYERS, D, F), jnp.float32) * D ** -0.5
    w_second = jax.random.normal(key_list[1], (LAYERS, F, D), jnp.float32) * (F ** -0.5 * BRANCH_SCALE)
    m_first = jax.random.normal(key_list[2], (LAYERS, D, F), jnp.float32) * (0.3 * BRANCH_SCALE / D)
    m_second = jax.random.normal(key_list[3], (LAYERS, F, D), jnp.float32) * (0.7 / D)
    return {'w_first': w_first, 'w_second': w_second, 'm_first': m_first, 'm_second': m_second,
            'x_now': draw_batch(key_list[4:7]), 'y_now': draw_batch(key_list[7:10]),
            'x_next': draw_batch(key_list[10:13]), 'y_next': draw_batch(key_list[13:16])}


def layer_stack(hidden, w_first_low, w_second_low):
    def body(carry, weights):
        pre_act = jnp.dot(carry.astype(jnp.bfloat16), weights[0], preferred_element_type=jnp.float32)
        act_low = jax.nn.gelu(pre_act).astype(jnp.bfloat16)
        return carry + jnp.dot(act_low, weights[1], preferred_element_type=jnp.float32), carry
    return lax.scan(body, hidden, (w_first_low, w_second_low))


def local_grads(rows_in, rows_target, w_first_low, w_second_low):
    h_last, h_saved = layer_stack(rows_in.astype(jnp.float32), w_first_low, w_second_low)
    grad_h = (h_last - rows_target.astype(jnp.float32)) / (BATCH * D)

    def back(grad_carry, layer_item):
        h_in, wf_low, ws_low = layer_item
        h_low = h_in.astype(jnp.bfloat16)
        pre_act = jnp.dot(h_low, wf_low, preferred_element_type=jnp.float32)
        act_val, gelu_back = jax.vjp(jax.nn.gelu, pre_act)
        act_low = act_val.astype(jnp.bfloat16)
        grad_low = grad_carry.astype(jnp.bfloat16)
        g_second = jnp.dot(act_low.T, grad_low, preferred_element_type=jnp.float32)
        grad_act = jnp.dot(grad_low, ws_low.T, preferred_element_type=jnp.float32)
        grad_pre = gelu_back(grad_act)[0].astype(jnp.bfloat16)
        g_first = jnp.dot(h_low.T, grad_pre, preferred_element_type=jnp.float32)
        grad_next = grad_carry + jnp.dot(grad_pre, wf_low.T, preferred_element_type=jnp.float32)
        return grad_next, (g_first.astype(jnp.bfloat16), g_second.astype(jnp.bfloat16))

    return lax.scan(back, grad_h, (h_saved, w_first_low, w_second_low), reverse=True)[1]


def reference(w_first, w_second, m_first, m_second, x_now, y_now, x_next, y_next):
    w_first_low = w_first.astype(jnp.bfloat16)
    w_second_low = w_second.astype(jnp.bfloat16)

    def add_device(grad_acc, rows_pair):
        g_first, g_second = local_grads(rows_pair[0], rows_pair[1], w_first_low, w_second_low)
        return (grad_acc[0] + g_first.astype(jnp.float32), grad_acc[1] + g_second.astype(jnp.float32)), None

    zero_acc = (jnp.zeros(w_first.shape, jnp.float32), jnp.zeros(w_second.shape, jnp.float32))
    rows_now = (x_now.reshape(DEVICES, TOK, D), y_now.reshape(DEVICES, TOK, D))
    (grad_first, grad_second), _ = lax.scan(add_device, zero_acc, rows_now)
    m_first_new = MOMENTUM * m_first + grad_first
    m_second_new = MOMENTUM * m_second + grad_second
    w_first_new = w_first - LEARN_RATE * m_first_new
    w_second_new = w_second - LEARN_RATE * m_second_new
    new_first_low = w_first_new.astype(jnp.bfloat16)
    new_second_low = w_second_new.astype(jnp.bfloat16)

    def next_device(rows_pair):
        h_last = layer_stack(rows_pair[0].astype(jnp.float32), new_first_low, new_second_low)[0]
        resid_rows = h_last - rows_pair[1].astype(jnp.float32)
        return h_last, jnp.sum(resid_rows * resid_rows, axis=-1) / (2 * D)

    rows_next = (x_next.reshape(DEVICES, TOK, D), y_next.reshape(DEVICES, TOK, D))
    h_out, loss_out = lax.map(next_device, rows_next)
    return (w_first_new, w_second_new, m_first_new, m_second_new,
            loss_out.reshape(BATCH), h_out.reshape(BATCH, D))
```

```python
import functools

import jax
import jax.numpy as jnp
from jax import lax
from jax.experimental import pallas as pl
from jax.experimental.pallas import tpu as pltpu
from jax.sharding import PartitionSpec as P

LEARN_BASE = 0.25
MOMENTUM = 0.9
C0 = 0.7978845608028654
C1 = C0 * 0.044715
MESH = pl.DeviceIdType.MESH
F32 = jnp.float32
BF16 = jnp.bfloat16
VMEM_LIMIT = 67_000_000

ORDERS = (("x", "y", "z"), ("y", "z", "x"), ("z", "x", "y"))
RING = 6
LAGS = (0, 1, 3, 4, 5, 6, 7, 9, 10)


def dot(a, b, ca=1, cb=0):
    return lax.dot_general(a, b, (((ca,), (cb,)), ((), ())), preferred_element_type=F32)


def gelu(a):
    t = jnp.tanh(a * (C0 + C1 * (a * a)))
    half = 0.5 * a
    return half + half * t


def gelu_both(a):
    a2 = a * a
    t = jnp.tanh(a * (C0 + C1 * a2))
    s = 0.5 + 0.5 * t
    u = a * s
    return u, s + u * (1.0 - s) * (2.0 * C0 + (6.0 * C1) * a2)


def layer_forward(h_ref, w1b_ref, w2b_ref, u_ref, hs_ref, chunk, tile):
    rows, width = h_ref.shape[0], w1b_ref.shape[1]
    for r in range(0, rows, chunk):
        hb = h_ref[r:r + chunk, :].astype(BF16)
        if hs_ref is not None:
            hs_ref[r:r + chunk, :] = hb
        for n in range(0, width, tile):
            u_ref[r:r + chunk, n:n + tile] = gelu(dot(hb, w1b_ref[:, n:n + tile])).astype(BF16)
        h_ref[r:r + chunk, :] = h_ref[r:r + chunk, :] + dot(u_ref[r:r + chunk, :], w2b_ref[...])


def forward_kernel(scale, x_ref, y_ref, w1_ref, w2_ref, hs_ref, w1b_ref, w2b_ref, g_ref, h_ref, u_ref):
    layer = pl.program_id(0)

    @pl.when(layer == 0)
    def _():
        h_ref[...] = x_ref[...].astype(F32)

    w1b_ref[...] = w1_ref[...].astype(BF16)
    w2b_ref[...] = w2_ref[...].astype(BF16)
    layer_forward(h_ref, w1b_ref, w2b_ref, u_ref, hs_ref, 256, 256)

    @pl.when(layer == pl.num_programs(0) - 1)
    def _():
        g_ref[...] = (h_ref[...] - y_ref[...].astype(F32)) * scale


def update_kernel(rate, x_ref, y_ref, w1_ref, w2_ref, m1_ref, m2_ref, gr_ref,
                  w1o_ref, w2o_ref, m1o_ref, m2o_ref, loss_ref, h_ref, w1b_ref, w2b_ref, u_ref):
    layer = pl.program_id(0)
    width = w1_ref.shape[0]

    @pl.when(layer == 0)
    def _():
        h_ref[...] = x_ref[...].astype(F32)

    mom = MOMENTUM * m1_ref[...] + gr_ref[:width, :].astype(F32)
    m1o_ref[...] = mom
    new = w1_ref[...] - rate * mom
    w1o_ref[...] = new
    w1b_ref[...] = new.astype(BF16)
    mom = MOMENTUM * m2_ref[...] + gr_ref[width:, :].astype(F32).T
    m2o_ref[...] = mom
    new = w2_ref[...] - rate * mom
    w2o_ref[...] = new
    w2b_ref[...] = new.astype(BF16)
    layer_forward(h_ref, w1b_ref, w2b_ref, u_ref, None, 256, 256)

    @pl.when(layer == pl.num_programs(0) - 1)
    def _():
        resid = h_ref[...] - y_ref[...].astype(F32)
        loss_ref[...] = jnp.sum((resid * resid).T, axis=0, keepdims=True) / (2 * width)


def backward_kernel(layers, g0_ref, w1_ref, w2_ref, hs_ref, out_ref,
                    g_ref, gb_ref, gt_ref, ht_ref, u_ref, q_ref,
                    grad_ref, sum_ref, r0_ref, r1_ref, r2_ref, r3_ref, send_sem, recv_sem, out_sem):
    it = pl.program_id(0)
    pod, data = lax.axis_index("pod"), lax.axis_index("data")
    z, y, x, c = pod // 2, pod % 2, data // 2, data % 2
    bits = {"x": x, "y": y, "z": z}
    peers = {
        "core": (pod, x * 2 + (1 - c)),
        "x": (pod, (1 - x) * 2 + c),
        "y": (z * 2 + (1 - y), data),
        "z": ((1 - z) * 2 + y, data),
    }
    rows, width = g_ref.shape
    hidden = u_ref.shape[1]
    block = 2 * width
    recv_refs = (r0_ref, r1_ref, r2_ref, r3_ref)
    third = hidden // 128 * 3 // 8 * 128
    parts = ((0, third), (third, third), (2 * third, hidden - 2 * third))

    @pl.when(it == 0)
    def _():
        barrier = pltpu.get_barrier_semaphore()
        for peer in peers.values():
            pl.semaphore_signal(barrier, inc=1, device_id=peer, device_id_type=MESH)
        pl.semaphore_wait(barrier, 4)
        g_ref[...] = g0_ref[...]

    def ring(slot):
        return slot % RING

    def region(part, k):
        offset = c * (block // 2)
        for n in range(k - 1):
            offset = offset + bits[ORDERS[part][n]] * (block >> (n + 2))
        return offset

    def message(slot, m, part):
        if m in (0, 7):
            size = block // 2
            mine, other = c * size, (1 - c) * size
            cols = slice(None)
            axis = "core"
            stage = 0
        else:
            stage = m if m <= 3 else 7 - m
            axis = ORDERS[part][stage - 1]
            size = block >> (stage + 1)
            base = region(part, stage)
            mine, other = base + bits[axis] * size, base + (1 - bits[axis]) * size
            cols = pl.ds(parts[part][0], parts[part][1])
        if m <= 3:
            src = grad_ref.at[ring(slot), pl.ds(pl.multiple_of(other, 16), size), cols]
            dst = recv_refs[stage].at[slot, :, cols]
        else:
            src = sum_ref.at[slot, pl.ds(pl.multiple_of(mine, 16), size), cols]
            dst = src
        return pltpu.make_async_remote_copy(
            src_ref=src, dst_ref=dst, send_sem=send_sem.at[slot, m, part], recv_sem=recv_sem.at[slot, m, part],
            device_id=peers[axis], device_id_type=MESH)

    def parts_of(m):
        return (0,) if m in (0, 7) else (0, 1, 2)

    def accumulate(slot, stage, part):
        size = block >> (stage + 1)
        if stage == 0:
            mine, cols = c * size, pl.ds(0, hidden)
        else:
            mine, cols = region(part, stage + 1), pl.ds(*parts[part])
        where = pl.ds(pl.multiple_of(mine, 16), size)
        total = grad_ref[ring(slot), where, cols].astype(F32) + recv_refs[stage][slot, :, cols].astype(F32)
        if stage == 3:
            sum_ref[slot, where, cols] = total.astype(BF16)
        else:
            grad_ref[ring(slot), where, cols] = total.astype(BF16)

    def result_copy(slot):
        return pltpu.make_async_copy(sum_ref.at[slot], out_ref.at[slot], out_sem.at[slot])

    def step(s, slot):
        if s > 0:
            m = s - 1
            for part in parts_of(m):
                message(slot, m, part).wait()
                if m <= 3:
                    accumulate(slot, m, part)
                if m not in (0, 7) and s < 8 and s != 7:
                    message(slot, s, part).start()
        if s == 0 or s == 1 or s == 7:
            for part in parts_of(s):
                message(slot, s, part).start()
        if s == 8:
            result_copy(slot).start()

    def comm_point(parity):
        for s in reversed(range(9)):
            if LAGS[s] % 2 == parity:
                done = it - 1 - (LAGS[s] - parity) // 2

                @pl.when(done >= 0)
                def _():
                    step(s, layers - 1 - done)

    tile, chunk = 256, 256
    comm_point(0)

    gb_ref[...] = g_ref[...].astype(BF16)
    gt_ref[...] = gb_ref[...].T
    ht_ref[...] = hs_ref[...].T

    def half(tiles):
        for n in tiles:
            cols = slice(n, n + tile)
            for r in range(0, rows, chunk):
                a = dot(hs_ref[r:r + chunk, :], w1_ref[:, cols])
                gu = dot(gb_ref[r:r + chunk, :], w2_ref[cols, :], 1, 1)
                u, slope = gelu_both(a)
                u_ref[r:r + chunk, cols] = u.astype(BF16)
                q_ref[r:r + chunk, cols] = (slope * gu).astype(BF16)
            layer = layers - 1 - it
            grad_ref[ring(layer), width:, cols] = dot(gt_ref[...], u_ref[:, cols]).astype(BF16)
            grad_ref[ring(layer), :width, cols] = dot(ht_ref[...], q_ref[:, cols]).astype(BF16)
            for r in range(0, rows, chunk):
                g_ref[r:r + chunk, :] = g_ref[r:r + chunk, :] + dot(q_ref[r:r + chunk, cols], w1_ref[:, cols], 1, 1)

    tiles = list(range(0, hidden, tile))
    half(tiles[:len(tiles) // 2])
    comm_point(1)
    half(tiles[len(tiles) // 2:])

    @pl.when(it == layers - 1)
    def _():
        for tick in range(2 * layers, 2 * layers + LAGS[8] + 1):
            for s in reversed(range(9)):
                if (tick - LAGS[s]) % 2 == 0:
                    done = (tick - 2 - LAGS[s]) // 2
                    if 0 <= done < layers:
                        step(s, layers - 1 - done)
        for slot in range(layers):
            result_copy(slot).wait()


def solution(mesh):
    n_pod = mesh.shape['pod']
    n_data = mesh.shape['data']
    rows_spec = P(('pod', 'data'), None)
    full_spec = P()

    def train_step(w_first, w_second, m_first, m_second, x_now, y_now, x_next, y_next):
        layers, width, hidden = w_first.shape
        rows = x_now.shape[0]
        batch = rows * n_pod * n_data
        whole = lambda *shape: pl.BlockSpec(shape, lambda i: (0,) * len(shape))
        per_layer = lambda *shape: pl.BlockSpec((None,) + shape, lambda i: (i, 0, 0))
        reverse = lambda *shape: pl.BlockSpec((None,) + shape, lambda i: (layers - 1 - i, 0, 0))
        shape = jax.ShapeDtypeStruct
        matmul_flops = 2 * rows * width * hidden * layers

        hs, w1b, w2b, g0 = pl.pallas_call(
            functools.partial(forward_kernel, 1.0 / (batch * width)),
            grid=(layers,),
            in_specs=[whole(rows, width), whole(rows, width), per_layer(width, hidden), per_layer(hidden, width)],
            out_specs=[per_layer(rows, width), per_layer(width, hidden), per_layer(hidden, width), whole(rows, width)],
            out_shape=[shape((layers, rows, width), BF16), shape((layers, width, hidden), BF16),
                       shape((layers, hidden, width), BF16), shape((rows, width), F32)],
            scratch_shapes=[pltpu.VMEM((rows, width), F32), pltpu.VMEM((rows, hidden), BF16)],
            compiler_params=pltpu.CompilerParams(dimension_semantics=("arbitrary",), vmem_limit_bytes=VMEM_LIMIT),
            cost_estimate=pl.CostEstimate(flops=2 * matmul_flops, bytes_accessed=60_000_000, transcendentals=0),
            name="forward_now",
        )(x_now, y_now, w_first, w_second)

        grads = pl.pallas_call(
            functools.partial(backward_kernel, layers),
            grid=(layers,),
            in_specs=[whole(rows, width), reverse(width, hidden), reverse(hidden, width), reverse(rows, width)],
            out_specs=pl.BlockSpec(memory_space=pl.ANY),
            out_shape=shape((layers, 2 * width, hidden), BF16),
            scratch_shapes=[
                pltpu.VMEM((rows, width), F32),
                pltpu.VMEM((rows, width), BF16),
                pltpu.VMEM((width, rows), BF16),
                pltpu.VMEM((width, rows), BF16),
                pltpu.VMEM((rows, hidden), BF16),
                pltpu.VMEM((rows, hidden), BF16),
                pltpu.VMEM((RING, 2 * width, hidden), BF16),
                pltpu.VMEM((layers, 2 * width, hidden), BF16),
                pltpu.VMEM((layers, width, hidden), BF16),
                pltpu.VMEM((layers, width // 2, hidden), BF16),
                pltpu.VMEM((layers, width // 4, hidden), BF16),
                pltpu.VMEM((layers, width // 8, hidden), BF16),
                pltpu.SemaphoreType.DMA((layers, 8, 3)),
                pltpu.SemaphoreType.DMA((layers, 8, 3)),
                pltpu.SemaphoreType.DMA((layers,)),
            ],
            compiler_params=pltpu.CompilerParams(dimension_semantics=("arbitrary",), vmem_limit_bytes=VMEM_LIMIT,
                                                 collective_id=0, has_side_effects=True),
            cost_estimate=pl.CostEstimate(flops=5 * matmul_flops, bytes_accessed=60_000_000, transcendentals=0),
            name="backward_reduce",
        )(g0, w1b, w2b, hs)

        outs = pl.pallas_call(
            functools.partial(update_kernel, LEARN_BASE / layers),
            grid=(layers,),
            in_specs=[whole(rows, width), whole(rows, width), per_layer(width, hidden), per_layer(hidden, width),
                      per_layer(width, hidden), per_layer(hidden, width), per_layer(2 * width, hidden)],
            out_specs=[per_layer(width, hidden), per_layer(hidden, width), per_layer(width, hidden),
                       per_layer(hidden, width), whole(1, rows), whole(rows, width)],
            out_shape=[shape((layers, width, hidden), F32), shape((layers, hidden, width), F32),
                       shape((layers, width, hidden), F32), shape((layers, hidden, width), F32),
                       shape((1, rows), F32), shape((rows, width), F32)],
            scratch_shapes=[pltpu.VMEM((width, hidden), BF16), pltpu.VMEM((hidden, width), BF16),
                            pltpu.VMEM((rows, hidden), BF16)],
            compiler_params=pltpu.CompilerParams(dimension_semantics=("arbitrary",), vmem_limit_bytes=VMEM_LIMIT),
            cost_estimate=pl.CostEstimate(flops=2 * matmul_flops, bytes_accessed=160_000_000, transcendentals=0),
            name="update_forward_next",
        )(x_next, y_next, w_first, w_second, m_first, m_second, grads)
        return outs[0], outs[1], outs[2], outs[3], outs[4].reshape(rows), outs[5]

    return jax.shard_map(train_step, mesh=mesh,
                         in_specs=(full_spec,) * 4 + (rows_spec,) * 4,
                         out_specs=(full_spec,) * 4 + (P(('pod', 'data')), rows_spec),
                         check_vma=False)
```

```python
import functools

import jax
import jax.numpy as jnp
from jax import lax
from jax.experimental import pallas as pl
from jax.experimental.pallas import tpu as pltpu
from jax.sharding import PartitionSpec as P

LEARN_BASE = 0.25
MOMENTUM = 0.9
C0 = 0.7978845608028654
C1 = C0 * 0.044715
H0, H1 = 2.0 * C0, 8.0 * C1
MESH = pl.DeviceIdType.MESH
F32 = jnp.float32
BF16 = jnp.bfloat16
VMEM_LIMIT = 67_000_000

LAGS = (0, 2, 4, 6, 7, 9, 11, 13, 15)
RING = 6
SLOTS = 6
AHEAD = 4


def dot(a, b, ca=1, cb=0):
    return lax.dot_general(a, b, (((ca,), (cb,)), ((), ())), preferred_element_type=F32)


def gelu(half):
    t = jnp.tanh(half * (H0 + H1 * (half * half)))
    return half + half * t


def gelu_both(half):
    sq = half * half
    t = jnp.tanh(half * (H0 + H1 * sq))
    s = 1.0 + t
    u = half * s
    return u, s + u * (1.0 - t) * (H0 + (3.0 * H1) * sq)


def layer_forward(h_ref, w1b_ref, w2b_ref, u_ref, hs_ref, chunk, tile):
    rows, width = h_ref.shape[0], w1b_ref.shape[1]
    for r in range(0, rows, chunk):
        hb = h_ref[r:r + chunk, :].astype(BF16)
        if hs_ref is not None:
            hs_ref[r:r + chunk, :] = hb
        for n in range(0, width, tile):
            u_ref[r:r + chunk, n:n + tile] = gelu(dot(hb, w1b_ref[:, n:n + tile])).astype(BF16)
        h_ref[r:r + chunk, :] = h_ref[r:r + chunk, :] + dot(u_ref[r:r + chunk, :], w2b_ref[...])


def forward_kernel(scale, x_ref, y_ref, w1_ref, w2_ref, hs_ref, w1b_ref, w2b_ref, g_ref, h_ref, u_ref):
    layer = pl.program_id(0)

    @pl.when(layer == 0)
    def _():
        h_ref[...] = x_ref[...].astype(F32)

    w1b_ref[...] = (0.5 * w1_ref[...]).astype(BF16)
    w2b_ref[...] = w2_ref[...].astype(BF16)
    layer_forward(h_ref, w1b_ref, w2b_ref, u_ref, hs_ref, 256, 256)

    @pl.when(layer == pl.num_programs(0) - 1)
    def _():
        g_ref[...] = (h_ref[...] - y_ref[...].astype(F32)) * scale


def update_kernel(rate, x_ref, y_ref, w1_hbm, w2_hbm, m1_hbm, m2_hbm, gr_hbm,
                  w1o_hbm, w2o_hbm, m1o_hbm, m2o_hbm, loss_ref, h_ref,
                  w1_ref, w2_ref, m1_ref, m2_ref, gr_ref, w1b_ref, w2b_ref, u_ref, in_sem, out_sem):
    layers, width = w1_hbm.shape[0], w1_hbm.shape[1]
    states = ((w1_hbm, w1_ref, w1o_hbm), (w2_hbm, w2_ref, w2o_hbm), (m1_hbm, m1_ref, m1o_hbm), (m2_hbm, m2_ref, m2o_hbm))

    def reads(layer):
        slot = layer % SLOTS
        pairs = [(src, buf) for src, buf, _ in states] + [(gr_hbm, gr_ref)]
        return [pltpu.make_async_copy(src.at[layer], buf.at[slot], in_sem.at[slot, n]) for n, (src, buf) in enumerate(pairs)]

    def writes(layer):
        slot = layer % SLOTS
        return [pltpu.make_async_copy(buf.at[slot], dst.at[layer], out_sem.at[slot, n])
                for n, (_, buf, dst) in enumerate(states)]

    for layer in range(AHEAD):
        for copy in reads(layer):
            copy.start()
    h_ref[...] = x_ref[...].astype(F32)

    @pl.loop(0, layers)
    def _(layer):
        slot = layer % SLOTS

        @pl.when(layer + AHEAD < layers)
        def _():
            @pl.when(layer + AHEAD >= SLOTS)
            def _():
                for copy in writes(layer + AHEAD - SLOTS):
                    copy.wait()
            for copy in reads(layer + AHEAD):
                copy.start()

        for copy in reads(layer):
            copy.wait()
        mom = MOMENTUM * m1_ref[slot] + gr_ref[slot, :width, :].astype(F32)
        m1_ref[slot] = mom
        new = w1_ref[slot] - rate * mom
        w1_ref[slot] = new
        w1b_ref[...] = (0.5 * new).astype(BF16)
        mom = MOMENTUM * m2_ref[slot] + gr_ref[slot, width:, :].astype(F32).T
        m2_ref[slot] = mom
        new = w2_ref[slot] - rate * mom
        w2_ref[slot] = new
        w2b_ref[...] = new.astype(BF16)
        for copy in writes(layer):
            copy.start()
        layer_forward(h_ref, w1b_ref, w2b_ref, u_ref, None, 256, 256)

    resid = h_ref[...] - y_ref[...].astype(F32)
    loss_ref[...] = jnp.sum((resid * resid).T, axis=0, keepdims=True) / (2 * width)
    for layer in range(layers - SLOTS, layers):
        for copy in writes(layer):
            copy.wait()


def backward_kernel(layers, g0_ref, w1_ref, w2_ref, hs_ref, out_ref,
                    g_ref, gb_ref, gt_ref, ht_ref, u_ref, q_ref,
                    grad_ref, sum_ref, r0_ref, r1_ref, r2_ref, r3_ref, send_sem, recv_sem, out_sem):
    it = pl.program_id(0)
    pod, data = lax.axis_index("pod"), lax.axis_index("data")
    z, y, x, c = pod // 2, pod % 2, data // 2, data % 2
    places = (x, y, z)
    neighbours = ((pod, (1 - x) * 2 + c), (z * 2 + (1 - y), data), ((1 - z) * 2 + y, data))
    sibling = (pod, x * 2 + (1 - c))
    rows, width = g_ref.shape
    hidden = u_ref.shape[1]
    block = 2 * width
    recv_refs = (r0_ref, r1_ref, r2_ref, r3_ref)
    third = hidden // 128 * 3 // 8 * 128
    parts = ((0, third), (third, third), (2 * third, hidden - 2 * third))

    @pl.when(it == 0)
    def _():
        barrier = pltpu.get_barrier_semaphore()
        for peer in neighbours + (sibling,):
            pl.semaphore_signal(barrier, inc=1, device_id=peer, device_id_type=MESH)
        pl.semaphore_wait(barrier, 4)
        g_ref[...] = g0_ref[...]

    def ring(slot):
        return slot % RING

    def pick(axis, options):
        weights = ((2 - axis) * (1 - axis) // 2, axis * (2 - axis), axis * (axis - 1) // 2)
        return sum(weight * option for weight, option in zip(weights, options))

    def axis_of(slot, part, stage):
        return (part + slot + stage - 1) % 3

    def region(slot, part, stage):
        offset = c * (block // 2)
        for n in range(1, stage + 1):
            offset = offset + pick(axis_of(slot, part, n), places) * (block >> (n + 1))
        return offset

    def message(slot, m, part):
        if m in (0, 7):
            stage, size, cols, peer = 0, block // 2, slice(None), sibling
            mine, other = c * size, (1 - c) * size
        else:
            stage = m if m <= 3 else 7 - m
            size, cols = block >> (stage + 1), pl.ds(*parts[part])
            axis = axis_of(slot, part, stage)
            place, base = pick(axis, places), region(slot, part, stage - 1)
            mine, other = base + place * size, base + (1 - place) * size
            peer = (pick(axis, [n[0] for n in neighbours]), pick(axis, [n[1] for n in neighbours]))
        if m <= 3:
            src = grad_ref.at[ring(slot), pl.ds(pl.multiple_of(other, 16), size), cols]
            dst = recv_refs[stage].at[slot, :, cols]
        else:
            src = sum_ref.at[slot, pl.ds(pl.multiple_of(mine, 16), size), cols]
            dst = src
        return pltpu.make_async_remote_copy(
            src_ref=src, dst_ref=dst, send_sem=send_sem.at[slot, m, part], recv_sem=recv_sem.at[slot, m, part],
            device_id=peer, device_id_type=MESH)

    def parts_of(m):
        return (0,) if m in (0, 7) else (0, 1, 2)

    def accumulate(slot, stage, part):
        size = block >> (stage + 1)
        if stage == 0:
            mine, cols = c * size, pl.ds(0, hidden)
        else:
            mine, cols = region(slot, part, stage), pl.ds(*parts[part])
        where = pl.ds(pl.multiple_of(mine, 16), size)
        total = grad_ref[ring(slot), where, cols].astype(F32) + recv_refs[stage][slot, :, cols].astype(F32)
        if stage == 3:
            sum_ref[slot, where, cols] = total.astype(BF16)
        else:
            grad_ref[ring(slot), where, cols] = total.astype(BF16)

    def result_copy(slot):
        return pltpu.make_async_copy(sum_ref.at[slot], out_ref.at[slot], out_sem.at[slot])

    def step(s, slot):
        if s > 0:
            m = s - 1
            for part in parts_of(m):
                message(slot, m, part).wait()
                if m <= 3:
                    accumulate(slot, m, part)
                if m not in (0, 7) and s < 8 and s != 7:
                    message(slot, s, part).start()
        if s == 0 or s == 1 or s == 7:
            for part in parts_of(s):
                message(slot, s, part).start()
        if s == 8:
            result_copy(slot).start()

    def comm_point(parity):
        for s in reversed(range(9)):
            if LAGS[s] % 2 == parity:
                done = it - 1 - (LAGS[s] - parity) // 2

                @pl.when(done >= 0)
                def _():
                    step(s, layers - 1 - done)

    tile, chunk = 256, 256
    comm_point(0)

    gb_ref[...] = g_ref[...].astype(BF16)
    gt_ref[...] = gb_ref[...].T
    ht_ref[...] = hs_ref[...].T

    def half(tiles):
        for n in tiles:
            cols = slice(n, n + tile)
            for r in range(0, rows, chunk):
                a = dot(hs_ref[r:r + chunk, :], w1_ref[:, cols])
                gu = dot(gb_ref[r:r + chunk, :], w2_ref[cols, :], 1, 1)
                u, slope = gelu_both(a)
                u_ref[r:r + chunk, cols] = u.astype(BF16)
                q_ref[r:r + chunk, cols] = (slope * gu).astype(BF16)
            layer = layers - 1 - it
            grad_ref[ring(layer), width:, cols] = (2.0 * dot(gt_ref[...], u_ref[:, cols])).astype(BF16)
            grad_ref[ring(layer), :width, cols] = dot(ht_ref[...], q_ref[:, cols]).astype(BF16)
            for r in range(0, rows, chunk):
                g_ref[r:r + chunk, :] = g_ref[r:r + chunk, :] + dot(q_ref[r:r + chunk, cols], w1_ref[:, cols], 1, 1)

    tiles = list(range(0, hidden, tile))
    half(tiles[:len(tiles) // 2])
    comm_point(1)
    half(tiles[len(tiles) // 2:])

    @pl.when(it == layers - 1)
    def _():
        taken = [sum(2 * n + 2 + lag < 2 * layers for lag in LAGS) for n in range(layers)]
        while min(taken) < 9:
            for n in reversed(range(layers)):
                if taken[n] < 9:
                    step(taken[n], layers - 1 - n)
                    taken[n] += 1
        for slot in range(layers):
            result_copy(slot).wait()


def solution(mesh):
    n_pod = mesh.shape['pod']
    n_data = mesh.shape['data']
    rows_spec = P(('pod', 'data'), None)
    full_spec = P()

    def train_step(w_first, w_second, m_first, m_second, x_now, y_now, x_next, y_next):
        layers, width, hidden = w_first.shape
        rows = x_now.shape[0]
        batch = rows * n_pod * n_data
        whole = lambda *shape: pl.BlockSpec(shape, lambda i: (0,) * len(shape))
        per_layer = lambda *shape: pl.BlockSpec((None,) + shape, lambda i: (i, 0, 0))
        reverse = lambda *shape: pl.BlockSpec((None,) + shape, lambda i: (layers - 1 - i, 0, 0))
        shape = jax.ShapeDtypeStruct
        matmul_flops = 2 * rows * width * hidden * layers

        hs, w1b, w2b, g0 = pl.pallas_call(
            functools.partial(forward_kernel, 0.5 / (batch * width)),
            grid=(layers,),
            in_specs=[whole(rows, width), whole(rows, width), per_layer(width, hidden), per_layer(hidden, width)],
            out_specs=[per_layer(rows, width), per_layer(width, hidden), per_layer(hidden, width), whole(rows, width)],
            out_shape=[shape((layers, rows, width), BF16), shape((layers, width, hidden), BF16),
                       shape((layers, hidden, width), BF16), shape((rows, width), F32)],
            scratch_shapes=[pltpu.VMEM((rows, width), F32), pltpu.VMEM((rows, hidden), BF16)],
            compiler_params=pltpu.CompilerParams(dimension_semantics=("arbitrary",), vmem_limit_bytes=VMEM_LIMIT),
            cost_estimate=pl.CostEstimate(flops=2 * matmul_flops, bytes_accessed=60_000_000, transcendentals=0),
            name="forward_now",
        )(x_now, y_now, w_first, w_second)

        grads = pl.pallas_call(
            functools.partial(backward_kernel, layers),
            grid=(layers,),
            in_specs=[whole(rows, width), reverse(width, hidden), reverse(hidden, width), reverse(rows, width)],
            out_specs=pl.BlockSpec(memory_space=pl.ANY),
            out_shape=shape((layers, 2 * width, hidden), BF16),
            scratch_shapes=[
                pltpu.VMEM((rows, width), F32),
                pltpu.VMEM((rows, width), BF16),
                pltpu.VMEM((width, rows), BF16),
                pltpu.VMEM((width, rows), BF16),
                pltpu.VMEM((rows, hidden), BF16),
                pltpu.VMEM((rows, hidden), BF16),
                pltpu.VMEM((RING, 2 * width, hidden), BF16),
                pltpu.VMEM((layers, 2 * width, hidden), BF16),
                pltpu.VMEM((layers, width, hidden), BF16),
                pltpu.VMEM((layers, width // 2, hidden), BF16),
                pltpu.VMEM((layers, width // 4, hidden), BF16),
                pltpu.VMEM((layers, width // 8, hidden), BF16),
                pltpu.SemaphoreType.DMA((layers, 8, 3)),
                pltpu.SemaphoreType.DMA((layers, 8, 3)),
                pltpu.SemaphoreType.DMA((layers,)),
            ],
            compiler_params=pltpu.CompilerParams(dimension_semantics=("arbitrary",), vmem_limit_bytes=VMEM_LIMIT,
                                                 collective_id=0, has_side_effects=True),
            cost_estimate=pl.CostEstimate(flops=5 * matmul_flops, bytes_accessed=60_000_000, transcendentals=0),
            name="backward_reduce",
        )(g0, w1b, w2b, hs)

        outs = pl.pallas_call(
            functools.partial(update_kernel, LEARN_BASE / layers),
            in_specs=[pl.BlockSpec(memory_space=pltpu.VMEM)] * 2 + [pl.BlockSpec(memory_space=pl.ANY)] * 5,
            out_specs=[pl.BlockSpec(memory_space=pl.ANY)] * 4 + [pl.BlockSpec(memory_space=pltpu.VMEM)] * 2,
            out_shape=[shape((layers, width, hidden), F32), shape((layers, hidden, width), F32),
                       shape((layers, width, hidden), F32), shape((layers, hidden, width), F32),
                       shape((1, rows), F32), shape((rows, width), F32)],
            scratch_shapes=[pltpu.VMEM((SLOTS, width, hidden), F32), pltpu.VMEM((SLOTS, hidden, width), F32),
                            pltpu.VMEM((SLOTS, width, hidden), F32), pltpu.VMEM((SLOTS, hidden, width), F32),
                            pltpu.VMEM((SLOTS, 2 * width, hidden), BF16),
                            pltpu.VMEM((width, hidden), BF16), pltpu.VMEM((hidden, width), BF16),
                            pltpu.VMEM((rows, hidden), BF16),
                            pltpu.SemaphoreType.DMA((SLOTS, 5)), pltpu.SemaphoreType.DMA((SLOTS, 4))],
            compiler_params=pltpu.CompilerParams(vmem_limit_bytes=VMEM_LIMIT),
            cost_estimate=pl.CostEstimate(flops=2 * matmul_flops, bytes_accessed=160_000_000, transcendentals=0),
            name="update_forward_next",
        )(x_next, y_next, w_first, w_second, m_first, m_second, grads)
        return outs[0], outs[1], outs[2], outs[3], outs[4].reshape(rows), outs[5]

    return jax.shard_map(train_step, mesh=mesh,
                         in_specs=(full_spec,) * 4 + (rows_spec,) * 4,
                         out_specs=(full_spec,) * 4 + (P(('pod', 'data')), rows_spec),
                         check_vma=False)
```

```python
import functools

import jax
import jax.numpy as jnp
from jax import lax
from jax.experimental import pallas as pl
from jax.experimental.pallas import tpu as pltpu
from jax.sharding import PartitionSpec as P

LEARN_BASE = 0.25
MOMENTUM = 0.9
C0 = 0.7978845608028654
C1 = C0 * 0.044715
H0, H1 = 2.0 * C0, 8.0 * C1
MESH = pl.DeviceIdType.MESH
F32 = jnp.float32
BF16 = jnp.bfloat16
VMEM_LIMIT = 67_000_000
BACK_LIMIT = 46 << 20
UPDATE_LIMIT = 26 << 20

LAGS = (0, 2, 4, 6, 7, 9, 11, 13, 15)
RING = 6
SLOTS = 5
AHEAD = 3


def dot(a, b, ca=1, cb=0):
    return lax.dot_general(a, b, (((ca,), (cb,)), ((), ())), preferred_element_type=F32)


def gelu(half):
    t = jnp.tanh(half * (H0 + H1 * (half * half)))
    return half + half * t


def gelu_both(half):
    sq = half * half
    t = jnp.tanh(half * (H0 + H1 * sq))
    s = 1.0 + t
    u = half * s
    return u, s + u * (1.0 - t) * (H0 + (3.0 * H1) * sq)


def layer_forward(h_ref, w1b_ref, w2b_ref, u_ref, hs_ref, chunk, tile):
    rows, width = h_ref.shape[0], w1b_ref.shape[1]
    for r in range(0, rows, chunk):
        hb = h_ref[r:r + chunk, :].astype(BF16)
        if hs_ref is not None:
            hs_ref[r:r + chunk, :] = hb
        for n in range(0, width, tile):
            u_ref[r:r + chunk, n:n + tile] = gelu(dot(hb, w1b_ref[:, n:n + tile])).astype(BF16)
        h_ref[r:r + chunk, :] = h_ref[r:r + chunk, :] + dot(u_ref[r:r + chunk, :], w2b_ref[...])


def forward_kernel(scale, x_ref, y_ref, w1_ref, w2_ref, hs_ref, w1b_ref, w2b_ref, g_ref, h_ref, u_ref):
    layer = pl.program_id(0)

    @pl.when(layer == 0)
    def _():
        h_ref[...] = x_ref[...].astype(F32)

    w1b_ref[...] = (0.5 * w1_ref[...]).astype(BF16)
    w2b_ref[...] = w2_ref[...].astype(BF16)
    layer_forward(h_ref, w1b_ref, w2b_ref, u_ref, hs_ref, 256, 256)

    @pl.when(layer == pl.num_programs(0) - 1)
    def _():
        g_ref[...] = (h_ref[...] - y_ref[...].astype(F32)) * scale


def update_kernel(rate, x_ref, y_ref, w1_hbm, w2_hbm, m1_hbm, m2_hbm, gr_ref,
                  w1o_hbm, w2o_hbm, m1o_hbm, m2o_hbm, loss_ref, h_ref,
                  w1_ref, w2_ref, m1_ref, m2_ref, w1b_ref, w2b_ref, u_ref, in_sem, out_sem):
    layers, width = w1_hbm.shape[0], w1_hbm.shape[1]
    states = ((w1_hbm, w1_ref, w1o_hbm), (w2_hbm, w2_ref, w2o_hbm), (m1_hbm, m1_ref, m1o_hbm), (m2_hbm, m2_ref, m2o_hbm))

    def reads(layer):
        slot = layer % SLOTS
        pairs = [(src, buf) for src, buf, _ in states]
        return [pltpu.make_async_copy(src.at[layer], buf.at[slot], in_sem.at[slot, n]) for n, (src, buf) in enumerate(pairs)]

    def writes(layer):
        slot = layer % SLOTS
        return [pltpu.make_async_copy(buf.at[slot], dst.at[layer], out_sem.at[slot, n])
                for n, (_, buf, dst) in enumerate(states)]

    for layer in range(AHEAD):
        for copy in reads(layer):
            copy.start()
    h_ref[...] = x_ref[...].astype(F32)

    @pl.loop(0, layers)
    def _(layer):
        slot = layer % SLOTS

        @pl.when(layer + AHEAD < layers)
        def _():
            @pl.when(layer + AHEAD >= SLOTS)
            def _():
                for copy in writes(layer + AHEAD - SLOTS):
                    copy.wait()
            for copy in reads(layer + AHEAD):
                copy.start()

        for copy in reads(layer):
            copy.wait()
        mom = MOMENTUM * m1_ref[slot] + gr_ref[layer, :width, :].astype(F32)
        m1_ref[slot] = mom
        new = w1_ref[slot] - rate * mom
        w1_ref[slot] = new
        w1b_ref[...] = (0.5 * new).astype(BF16)
        mom = MOMENTUM * m2_ref[slot] + gr_ref[layer, width:, :].astype(F32).T
        m2_ref[slot] = mom
        new = w2_ref[slot] - rate * mom
        w2_ref[slot] = new
        w2b_ref[...] = new.astype(BF16)
        for copy in writes(layer):
            copy.start()
        layer_forward(h_ref, w1b_ref, w2b_ref, u_ref, None, 256, 256)

    resid = h_ref[...] - y_ref[...].astype(F32)
    loss_ref[...] = jnp.sum((resid * resid).T, axis=0, keepdims=True) / (2 * width)
    for layer in range(layers - SLOTS, layers):
        for copy in writes(layer):
            copy.wait()


def backward_kernel(g0_ref, w1_hbm, w2_hbm, hs_hbm, sum_ref, w1_buf, w2_buf, hs_buf, in_sem,
                    g_ref, gb_ref, gt_ref, ht_ref, u_ref, q_ref,
                    grad_ref, r0_ref, r1_ref, r2_ref, r3_ref, send_sem, recv_sem):
    layers = w1_hbm.shape[0]
    pod, data = lax.axis_index("pod"), lax.axis_index("data")
    z, y, x, c = pod // 2, pod % 2, data // 2, data % 2
    places = (x, y, z)
    neighbours = ((pod, (1 - x) * 2 + c), (z * 2 + (1 - y), data), ((1 - z) * 2 + y, data))
    sibling = (pod, x * 2 + (1 - c))
    rows, width = g_ref.shape
    hidden = u_ref.shape[1]
    block = 2 * width
    recv_refs = (r0_ref, r1_ref, r2_ref, r3_ref)
    third = hidden // 128 * 3 // 8 * 128
    parts = ((0, third), (third, third), (2 * third, hidden - 2 * third))

    def reads(it):
        slot, layer = it % 2, layers - 1 - it
        pairs = ((w1_hbm, w1_buf), (w2_hbm, w2_buf), (hs_hbm, hs_buf))
        return [pltpu.make_async_copy(src.at[layer], buf.at[slot], in_sem.at[slot, n]) for n, (src, buf) in enumerate(pairs)]

    for copy in reads(0):
        copy.start()
    barrier = pltpu.get_barrier_semaphore()
    for peer in neighbours + (sibling,):
        pl.semaphore_signal(barrier, inc=1, device_id=peer, device_id_type=MESH)
    pl.semaphore_wait(barrier, 4)
    g_ref[...] = g0_ref[...]

    def ring(slot):
        return slot % RING

    def pick(axis, options):
        weights = ((2 - axis) * (1 - axis) // 2, axis * (2 - axis), axis * (axis - 1) // 2)
        return sum(weight * option for weight, option in zip(weights, options))

    def axis_of(slot, part, stage):
        return (part + slot + stage - 1) % 3

    def region(slot, part, stage):
        offset = c * (block // 2)
        for n in range(1, stage + 1):
            offset = offset + pick(axis_of(slot, part, n), places) * (block >> (n + 1))
        return offset

    def message(slot, m, part):
        if m in (0, 7):
            stage, size, cols, peer = 0, block // 2, slice(None), sibling
            mine, other = c * size, (1 - c) * size
        else:
            stage = m if m <= 3 else 7 - m
            size, cols = block >> (stage + 1), pl.ds(*parts[part])
            axis = axis_of(slot, part, stage)
            place, base = pick(axis, places), region(slot, part, stage - 1)
            mine, other = base + place * size, base + (1 - place) * size
            peer = (pick(axis, [n[0] for n in neighbours]), pick(axis, [n[1] for n in neighbours]))
        if m <= 3:
            src = grad_ref.at[ring(slot), pl.ds(pl.multiple_of(other, 16), size), cols]
            dst = recv_refs[stage].at[slot, :, cols]
        else:
            src = sum_ref.at[slot, pl.ds(pl.multiple_of(mine, 16), size), cols]
            dst = src
        return pltpu.make_async_remote_copy(
            src_ref=src, dst_ref=dst, send_sem=send_sem.at[slot, m, part], recv_sem=recv_sem.at[slot, m, part],
            device_id=peer, device_id_type=MESH)

    def parts_of(m):
        return (0,) if m in (0, 7) else (0, 1, 2)

    def accumulate(slot, stage, part):
        size = block >> (stage + 1)
        if stage == 0:
            mine, cols = c * size, pl.ds(0, hidden)
        else:
            mine, cols = region(slot, part, stage), pl.ds(*parts[part])
        where = pl.ds(pl.multiple_of(mine, 16), size)
        total = grad_ref[ring(slot), where, cols].astype(F32) + recv_refs[stage][slot, :, cols].astype(F32)
        if stage == 3:
            sum_ref[slot, where, cols] = total.astype(BF16)
        else:
            grad_ref[ring(slot), where, cols] = total.astype(BF16)

    def step(s, slot):
        if s > 0:
            m = s - 1
            for part in parts_of(m):
                message(slot, m, part).wait()
                if m <= 3:
                    accumulate(slot, m, part)
                if m not in (0, 7) and s < 8 and s != 7:
                    message(slot, s, part).start()
        if s == 0 or s == 1 or s == 7:
            for part in parts_of(s):
                message(slot, s, part).start()

    def comm_point(it, parity):
        for s in reversed(range(9)):
            if LAGS[s] % 2 == parity:
                done = it - 1 - (LAGS[s] - parity) // 2

                @pl.when(done >= 0)
                def _():
                    step(s, layers - 1 - done)

    tile, chunk = 256, 256

    @pl.loop(0, layers)
    def _(it):
        comm_point(it, 0)

        @pl.when(it + 1 < layers)
        def _():
            for copy in reads(it + 1):
                copy.start()

        for copy in reads(it):
            copy.wait()
        w1_ref, w2_ref, hs_ref = (buf.at[it % 2] for buf in (w1_buf, w2_buf, hs_buf))

        gb_ref[...] = g_ref[...].astype(BF16)
        gt_ref[...] = gb_ref[...].T
        ht_ref[...] = hs_ref[...].T

        layer = layers - 1 - it

        def first(n, r):
            cols = slice(n, n + tile)
            a = dot(hs_ref[r:r + chunk, :], w1_ref[:, cols])
            gu = dot(gb_ref[r:r + chunk, :], w2_ref[cols, :], 1, 1)
            u, slope = gelu_both(a)
            u_ref[r:r + chunk, cols] = u.astype(BF16)
            q_ref[r:r + chunk, cols] = (slope * gu).astype(BF16)

        def carry(n, r):
            cols = slice(n, n + tile)
            g_ref[r:r + chunk, :] = g_ref[r:r + chunk, :] + dot(q_ref[r:r + chunk, cols], w1_ref[:, cols], 1, 1)

        def grad_second(n):
            cols = slice(n, n + tile)
            grad_ref[ring(layer), width:, cols] = (2.0 * dot(gt_ref[...], u_ref[:, cols])).astype(BF16)

        def grad_first(n):
            cols = slice(n, n + tile)
            grad_ref[ring(layer), :width, cols] = dot(ht_ref[...], q_ref[:, cols]).astype(BF16)

        def tile_step(n, previous):
            for i, r in enumerate(range(0, rows, chunk)):
                if previous is not None:
                    carry(previous, r)
                    if i == rows // chunk // 2 - 1:
                        grad_second(previous)
                if n is not None:
                    first(n, r)
            if previous is not None:
                grad_first(previous)

        tiles = list(range(0, hidden, tile)) + [None]
        for i, n in enumerate(tiles):
            if i == len(tiles) // 2:
                comm_point(it, 1)
            tile_step(n, tiles[i - 1] if i > 0 else None)

    taken = [sum(2 * n + 2 + lag < 2 * layers for lag in LAGS) for n in range(layers)]
    while min(taken) < 9:
        for n in reversed(range(layers)):
            if taken[n] < 9:
                step(taken[n], layers - 1 - n)
                taken[n] += 1


def solution(mesh):
    n_pod = mesh.shape['pod']
    n_data = mesh.shape['data']
    rows_spec = P(('pod', 'data'), None)
    full_spec = P()

    def train_step(w_first, w_second, m_first, m_second, x_now, y_now, x_next, y_next):
        layers, width, hidden = w_first.shape
        rows = x_now.shape[0]
        batch = rows * n_pod * n_data
        whole = lambda *shape: pl.BlockSpec(shape, lambda i: (0,) * len(shape))
        per_layer = lambda *shape: pl.BlockSpec((None,) + shape, lambda i: (i, 0, 0))
        shape = jax.ShapeDtypeStruct
        matmul_flops = 2 * rows * width * hidden * layers

        hs, w1b, w2b, g0 = pl.pallas_call(
            functools.partial(forward_kernel, 0.5 / (batch * width)),
            grid=(layers,),
            in_specs=[whole(rows, width), whole(rows, width), per_layer(width, hidden), per_layer(hidden, width)],
            out_specs=[per_layer(rows, width), per_layer(width, hidden), per_layer(hidden, width), whole(rows, width)],
            out_shape=[shape((layers, rows, width), BF16), shape((layers, width, hidden), BF16),
                       shape((layers, hidden, width), BF16), shape((rows, width), F32)],
            scratch_shapes=[pltpu.VMEM((rows, width), F32), pltpu.VMEM((rows, hidden), BF16)],
            compiler_params=pltpu.CompilerParams(dimension_semantics=("arbitrary",), vmem_limit_bytes=VMEM_LIMIT),
            cost_estimate=pl.CostEstimate(flops=2 * matmul_flops, bytes_accessed=60_000_000, transcendentals=0),
            name="forward_now",
        )(x_now, y_now, w_first, w_second)

        grads = pl.pallas_call(
            backward_kernel,
            in_specs=[pl.BlockSpec(memory_space=pltpu.VMEM)] + [pl.BlockSpec(memory_space=pl.ANY)] * 3,
            out_specs=pl.BlockSpec(memory_space=pltpu.VMEM),
            out_shape=pltpu.VMEM((layers, 2 * width, hidden), BF16),
            scratch_shapes=[
                pltpu.VMEM((2, width, hidden), BF16),
                pltpu.VMEM((2, hidden, width), BF16),
                pltpu.VMEM((2, rows, width), BF16),
                pltpu.SemaphoreType.DMA((2, 3)),
                pltpu.VMEM((rows, width), F32),
                pltpu.VMEM((rows, width), BF16),
                pltpu.VMEM((width, rows), BF16),
                pltpu.VMEM((width, rows), BF16),
                pltpu.VMEM((rows, hidden), BF16),
                pltpu.VMEM((rows, hidden), BF16),
                pltpu.VMEM((RING, 2 * width, hidden), BF16),
                pltpu.VMEM((layers, width, hidden), BF16),
                pltpu.VMEM((layers, width // 2, hidden), BF16),
                pltpu.VMEM((layers, width // 4, hidden), BF16),
                pltpu.VMEM((layers, width // 8, hidden), BF16),
                pltpu.SemaphoreType.DMA((layers, 8, 3)),
                pltpu.SemaphoreType.DMA((layers, 8, 3)),
            ],
            compiler_params=pltpu.CompilerParams(vmem_limit_bytes=BACK_LIMIT,
                                                 collective_id=0, has_side_effects=True),
            cost_estimate=pl.CostEstimate(flops=5 * matmul_flops, bytes_accessed=60_000_000, transcendentals=0),
            name="backward_reduce",
        )(g0, w1b, w2b, hs)

        outs = pl.pallas_call(
            functools.partial(update_kernel, LEARN_BASE / layers),
            in_specs=[pl.BlockSpec(memory_space=pltpu.VMEM)] * 2 + [pl.BlockSpec(memory_space=pl.ANY)] * 4 +
                     [pl.BlockSpec(memory_space=pltpu.VMEM)],
            out_specs=[pl.BlockSpec(memory_space=pl.ANY)] * 4 + [pl.BlockSpec(memory_space=pltpu.VMEM)] * 2,
            out_shape=[shape((layers, width, hidden), F32), shape((layers, hidden, width), F32),
                       shape((layers, width, hidden), F32), shape((layers, hidden, width), F32),
                       shape((1, rows), F32), shape((rows, width), F32)],
            scratch_shapes=[pltpu.VMEM((SLOTS, width, hidden), F32), pltpu.VMEM((SLOTS, hidden, width), F32),
                            pltpu.VMEM((SLOTS, width, hidden), F32), pltpu.VMEM((SLOTS, hidden, width), F32),
                            pltpu.VMEM((width, hidden), BF16), pltpu.VMEM((hidden, width), BF16),
                            pltpu.VMEM((rows, hidden), BF16),
                            pltpu.SemaphoreType.DMA((SLOTS, 4)), pltpu.SemaphoreType.DMA((SLOTS, 4))],
            compiler_params=pltpu.CompilerParams(vmem_limit_bytes=UPDATE_LIMIT),
            cost_estimate=pl.CostEstimate(flops=2 * matmul_flops, bytes_accessed=160_000_000, transcendentals=0),
            name="update_forward_next",
        )(x_next, y_next, w_first, w_second, m_first, m_second, pltpu.with_memory_space_constraint(grads, pltpu.VMEM))
        return outs[0], outs[1], outs[2], outs[3], outs[4].reshape(rows), outs[5]

    return jax.shard_map(train_step, mesh=mesh,
                         in_specs=(full_spec,) * 4 + (rows_spec,) * 4,
                         out_specs=(full_spec,) * 4 + (P(('pod', 'data')), rows_spec),
                         check_vma=False)
```

```python
import functools

import jax
import jax.numpy as jnp
from jax import lax
from jax.experimental import pallas as pl
from jax.experimental.pallas import tpu as pltpu
from jax.sharding import PartitionSpec as P

LEARN_BASE = 0.25
MOMENTUM = 0.9
C0 = 0.7978845608028654
C1 = C0 * 0.044715
H0, H1 = 2.0 * C0, 8.0 * C1
MESH = pl.DeviceIdType.MESH
F32 = jnp.float32
BF16 = jnp.bfloat16
BACK_LIMIT = 46 << 20
UPDATE_LIMIT = 26 << 20

LOADS = 3
LAGS = (0, 2, 4, 6, 7, 9, 11, 13, 15)
RING = 6
SLOTS = 5
AHEAD = 3


def dot(a, b, ca=1, cb=0):
    return lax.dot_general(a, b, (((ca,), (cb,)), ((), ())), preferred_element_type=F32)


def gelu(half):
    t = jnp.tanh(half * (H0 + H1 * (half * half)))
    return half + half * t


def gelu_both(half):
    sq = half * half
    t = jnp.tanh(half * (H0 + H1 * sq))
    s = 1.0 + t
    u = half * s
    return u, s + u * (1.0 - t) * (H0 + (3.0 * H1) * sq)


def layer_forward(h_ref, w1b_ref, w2b_ref, u_ref, hs_ref, chunk, tile):
    rows, width = h_ref.shape[0], w1b_ref.shape[1]
    for r in range(0, rows, chunk):
        hb = h_ref[r:r + chunk, :].astype(BF16)
        if hs_ref is not None:
            hs_ref[r:r + chunk, :] = hb
        for n in range(0, width, tile):
            u_ref[r:r + chunk, n:n + tile] = gelu(dot(hb, w1b_ref[:, n:n + tile])).astype(BF16)
        h_ref[r:r + chunk, :] = h_ref[r:r + chunk, :] + dot(u_ref[r:r + chunk, :], w2b_ref[...])


def update_kernel(rate, x_ref, y_ref, w1_hbm, w2_hbm, m1_hbm, m2_hbm, gr_ref,
                  w1o_hbm, w2o_hbm, m1o_hbm, m2o_hbm, loss_ref, h_ref,
                  w1_ref, w2_ref, m1_ref, m2_ref, w1b_ref, w2b_ref, u_ref, in_sem, out_sem):
    layers, width = w1_hbm.shape[0], w1_hbm.shape[1]
    states = ((w1_hbm, w1_ref, w1o_hbm), (w2_hbm, w2_ref, w2o_hbm), (m1_hbm, m1_ref, m1o_hbm), (m2_hbm, m2_ref, m2o_hbm))

    def reads(layer):
        slot = layer % SLOTS
        pairs = [(src, buf) for src, buf, _ in states]
        return [pltpu.make_async_copy(src.at[layer], buf.at[slot], in_sem.at[slot, n]) for n, (src, buf) in enumerate(pairs)]

    def writes(layer):
        slot = layer % SLOTS
        return [pltpu.make_async_copy(buf.at[slot], dst.at[layer], out_sem.at[slot, n])
                for n, (_, buf, dst) in enumerate(states)]

    for layer in range(AHEAD):
        for copy in reads(layer):
            copy.start()
    h_ref[...] = x_ref[...].astype(F32)

    @pl.loop(0, layers)
    def _(layer):
        slot = layer % SLOTS

        @pl.when(layer + AHEAD < layers)
        def _():
            @pl.when(layer + AHEAD >= SLOTS)
            def _():
                for copy in writes(layer + AHEAD - SLOTS):
                    copy.wait()
            for copy in reads(layer + AHEAD):
                copy.start()

        for copy in reads(layer):
            copy.wait()
        mom = MOMENTUM * m1_ref[slot] + gr_ref[layer, :width, :].astype(F32)
        m1_ref[slot] = mom
        new = w1_ref[slot] - rate * mom
        w1_ref[slot] = new
        w1b_ref[...] = (0.5 * new).astype(BF16)
        mom = MOMENTUM * m2_ref[slot] + gr_ref[layer, width:, :].astype(F32).T
        m2_ref[slot] = mom
        new = w2_ref[slot] - rate * mom
        w2_ref[slot] = new
        w2b_ref[...] = new.astype(BF16)
        for copy in writes(layer):
            copy.start()
        layer_forward(h_ref, w1b_ref, w2b_ref, u_ref, None, 512, 256)

    resid = h_ref[...] - y_ref[...].astype(F32)
    loss_ref[...] = jnp.sum((resid * resid).T, axis=0, keepdims=True) / (2 * width)
    for layer in range(layers - SLOTS, layers):
        for copy in writes(layer):
            copy.wait()


def gradient_kernel(scale, x_ref, y_ref, w1f_hbm, w2f_hbm, sum_ref, w1_hbm, w2_hbm, hs_hbm,
                    w1f_buf, w2f_buf, w1_buf, w2_buf, hs_buf, load_sem, save_sem, in_sem, g_ref, gb_ref, gt_ref, ht_ref, u_ref, q_ref,
                    grad_ref, r0_ref, r1_ref, r2_ref, r3_ref, send_sem, recv_sem):
    layers = w1f_hbm.shape[0]
    pod, data = lax.axis_index("pod"), lax.axis_index("data")
    z, y, x, c = pod // 2, pod % 2, data // 2, data % 2
    places = (x, y, z)
    neighbours = ((pod, (1 - x) * 2 + c), (z * 2 + (1 - y), data), ((1 - z) * 2 + y, data))
    sibling = (pod, x * 2 + (1 - c))
    rows, width = g_ref.shape
    hidden = u_ref.shape[1]
    block = 2 * width
    recv_refs = (r0_ref, r1_ref, r2_ref, r3_ref)
    third = hidden // 128 * 3 // 8 * 128
    parts = ((0, third), (third, third), (2 * third, hidden - 2 * third))

    saved = ((w1_hbm, w1_buf), (w2_hbm, w2_buf), (hs_hbm, hs_buf))

    def loads(layer):
        slot = layer % LOADS
        return [pltpu.make_async_copy(src.at[layer], buf.at[slot], load_sem.at[slot, n])
                for n, (src, buf) in enumerate(((w1f_hbm, w1f_buf), (w2f_hbm, w2f_buf)))]

    def saves(layer):
        slot = layer % 2
        return [pltpu.make_async_copy(buf.at[slot], dst.at[layer], save_sem.at[slot, n]) for n, (dst, buf) in enumerate(saved)]

    def reads(layer):
        slot = layer % 2
        return [pltpu.make_async_copy(src.at[layer], buf.at[slot], in_sem.at[slot, n]) for n, (src, buf) in enumerate(saved)]

    for layer in range(LOADS - 1):
        for copy in loads(layer):
            copy.start()
    barrier = pltpu.get_barrier_semaphore()
    for peer in neighbours + (sibling,):
        pl.semaphore_signal(barrier, inc=1, device_id=peer, device_id_type=MESH)
    g_ref[...] = x_ref[...].astype(F32)

    @pl.loop(0, layers)
    def _(layer):
        slot = layer % 2

        @pl.when(layer + LOADS - 1 < layers)
        def _():
            for copy in loads(layer + LOADS - 1):
                copy.start()

        @pl.when(layer >= 2)
        def _():
            for copy in saves(layer - 2):
                copy.wait()

        for copy in loads(layer):
            copy.wait()
        w1_buf[slot] = (0.5 * w1f_buf[layer % LOADS]).astype(BF16)
        w2_buf[slot] = w2f_buf[layer % LOADS].astype(BF16)
        layer_forward(g_ref, w1_buf.at[slot], w2_buf.at[slot], u_ref, hs_buf.at[slot], 512, 256)

        @pl.when(layer < layers - 2)
        def _():
            for copy in saves(layer):
                copy.start()

    g_ref[...] = (g_ref[...] - y_ref[...].astype(F32)) * scale
    pl.semaphore_wait(barrier, 4)

    def ring(slot):
        return slot % RING

    def pick(axis, options):
        weights = ((2 - axis) * (1 - axis) // 2, axis * (2 - axis), axis * (axis - 1) // 2)
        return sum(weight * option for weight, option in zip(weights, options))

    def axis_of(slot, part, stage):
        return (part + slot + stage - 1) % 3

    def region(slot, part, stage):
        offset = c * (block // 2)
        for n in range(1, stage + 1):
            offset = offset + pick(axis_of(slot, part, n), places) * (block >> (n + 1))
        return offset

    def message(slot, m, part):
        if m in (0, 7):
            stage, size, cols, peer = 0, block // 2, slice(None), sibling
            mine, other = c * size, (1 - c) * size
        else:
            stage = m if m <= 3 else 7 - m
            size, cols = block >> (stage + 1), pl.ds(*parts[part])
            axis = axis_of(slot, part, stage)
            place, base = pick(axis, places), region(slot, part, stage - 1)
            mine, other = base + place * size, base + (1 - place) * size
            peer = (pick(axis, [n[0] for n in neighbours]), pick(axis, [n[1] for n in neighbours]))
        if m <= 3:
            src = grad_ref.at[ring(slot), pl.ds(pl.multiple_of(other, 16), size), cols]
            dst = recv_refs[stage].at[slot, :, cols]
        else:
            src = sum_ref.at[slot, pl.ds(pl.multiple_of(mine, 16), size), cols]
            dst = src
        return pltpu.make_async_remote_copy(
            src_ref=src, dst_ref=dst, send_sem=send_sem.at[slot, m, part], recv_sem=recv_sem.at[slot, m, part],
            device_id=peer, device_id_type=MESH)

    def parts_of(m):
        return (0,) if m in (0, 7) else (0, 1, 2)

    def accumulate(slot, stage, part):
        size = block >> (stage + 1)
        if stage == 0:
            mine, cols = c * size, pl.ds(0, hidden)
        else:
            mine, cols = region(slot, part, stage), pl.ds(*parts[part])
        where = pl.ds(pl.multiple_of(mine, 16), size)
        total = grad_ref[ring(slot), where, cols].astype(F32) + recv_refs[stage][slot, :, cols].astype(F32)
        if stage == 3:
            sum_ref[slot, where, cols] = total.astype(BF16)
        else:
            grad_ref[ring(slot), where, cols] = total.astype(BF16)

    def step(s, slot):
        if s > 0:
            m = s - 1
            for part in parts_of(m):
                message(slot, m, part).wait()
                if m <= 3:
                    accumulate(slot, m, part)
                if m not in (0, 7) and s < 8 and s != 7:
                    message(slot, s, part).start()
        if s == 0 or s == 1 or s == 7:
            for part in parts_of(s):
                message(slot, s, part).start()

    def comm_point(it, parity):
        for s in reversed(range(9)):
            if LAGS[s] % 2 == parity:
                done = it - 1 - (LAGS[s] - parity) // 2

                @pl.when(done >= 0)
                def _():
                    step(s, layers - 1 - done)

    tile, chunk = 256, 256

    @pl.loop(0, layers)
    def _(it):
        comm_point(it, 0)

        layer = layers - 1 - it

        @pl.when((it >= 1) & (it + 1 < layers))
        def _():
            for copy in reads(layer - 1):
                copy.start()

        @pl.when(it >= 2)
        def _():
            for copy in reads(layer):
                copy.wait()

        w1_ref, w2_ref, hs_ref = (buf.at[layer % 2] for buf in (w1_buf, w2_buf, hs_buf))

        gb_ref[...] = g_ref[...].astype(BF16)
        gt_ref[...] = gb_ref[...].T
        ht_ref[...] = hs_ref[...].T

        def first(n, r):
            cols = slice(n, n + tile)
            a = dot(hs_ref[r:r + chunk, :], w1_ref[:, cols])
            gu = dot(gb_ref[r:r + chunk, :], w2_ref[cols, :], 1, 1)
            u, slope = gelu_both(a)
            u_ref[r:r + chunk, cols] = u.astype(BF16)
            q_ref[r:r + chunk, cols] = (slope * gu).astype(BF16)

        def carry(n, r):
            cols = slice(n, n + tile)
            g_ref[r:r + chunk, :] = g_ref[r:r + chunk, :] + dot(q_ref[r:r + chunk, cols], w1_ref[:, cols], 1, 1)

        def grad_second(n):
            cols = slice(n, n + tile)
            grad_ref[ring(layer), width:, cols] = (2.0 * dot(gt_ref[...], u_ref[:, cols])).astype(BF16)

        def grad_first(n):
            cols = slice(n, n + tile)
            grad_ref[ring(layer), :width, cols] = dot(ht_ref[...], q_ref[:, cols]).astype(BF16)

        def tile_step(n, previous):
            for i, r in enumerate(range(0, rows, chunk)):
                if previous is not None:
                    carry(previous, r)
                    if i == rows // chunk // 2 - 1:
                        grad_second(previous)
                if n is not None:
                    first(n, r)
            if previous is not None:
                grad_first(previous)

        tiles = list(range(0, hidden, tile)) + [None]
        for i, n in enumerate(tiles):
            if i == len(tiles) // 2:
                comm_point(it, 1)
            tile_step(n, tiles[i - 1] if i > 0 else None)

    taken = [sum(2 * n + 2 + lag < 2 * layers for lag in LAGS) for n in range(layers)]
    while min(taken) < 9:
        for n in reversed(range(layers)):
            if taken[n] < 9:
                step(taken[n], layers - 1 - n)
                taken[n] += 1


def solution(mesh):
    n_pod = mesh.shape['pod']
    n_data = mesh.shape['data']
    rows_spec = P(('pod', 'data'), None)
    full_spec = P()

    def train_step(w_first, w_second, m_first, m_second, x_now, y_now, x_next, y_next):
        layers, width, hidden = w_first.shape
        rows = x_now.shape[0]
        batch = rows * n_pod * n_data
        shape = jax.ShapeDtypeStruct
        matmul_flops = 2 * rows * width * hidden * layers

        grads = pl.pallas_call(
            functools.partial(gradient_kernel, 0.5 / (batch * width)),
            in_specs=[pl.BlockSpec(memory_space=pltpu.VMEM)] * 2 + [pl.BlockSpec(memory_space=pl.ANY)] * 2,
            out_specs=[pl.BlockSpec(memory_space=pltpu.VMEM)] + [pl.BlockSpec(memory_space=pl.ANY)] * 3,
            out_shape=[pltpu.VMEM((layers, 2 * width, hidden), BF16), shape((layers - 2, width, hidden), BF16),
                       shape((layers - 2, hidden, width), BF16), shape((layers - 2, rows, width), BF16)],
            scratch_shapes=[
                pltpu.VMEM((LOADS, width, hidden), F32),
                pltpu.VMEM((LOADS, hidden, width), F32),
                pltpu.VMEM((2, width, hidden), BF16),
                pltpu.VMEM((2, hidden, width), BF16),
                pltpu.VMEM((2, rows, width), BF16),
                pltpu.SemaphoreType.DMA((LOADS, 2)),
                pltpu.SemaphoreType.DMA((2, 3)),
                pltpu.SemaphoreType.DMA((2, 3)),
                pltpu.VMEM((rows, width), F32),
                pltpu.VMEM((rows, width), BF16),
                pltpu.VMEM((width, rows), BF16),
                pltpu.VMEM((width, rows), BF16),
                pltpu.VMEM((rows, hidden), BF16),
                pltpu.VMEM((rows, hidden), BF16),
                pltpu.VMEM((RING, 2 * width, hidden), BF16),
                pltpu.VMEM((layers, width, hidden), BF16),
                pltpu.VMEM((layers, width // 2, hidden), BF16),
                pltpu.VMEM((layers, width // 4, hidden), BF16),
                pltpu.VMEM((layers, width // 8, hidden), BF16),
                pltpu.SemaphoreType.DMA((layers, 8, 3)),
                pltpu.SemaphoreType.DMA((layers, 8, 3)),
            ],
            compiler_params=pltpu.CompilerParams(vmem_limit_bytes=BACK_LIMIT,
                                                 collective_id=0, has_side_effects=True),
            cost_estimate=pl.CostEstimate(flops=7 * matmul_flops, bytes_accessed=80_000_000, transcendentals=0),
            name="gradient",
        )(x_now, y_now, w_first, w_second)[0]

        outs = pl.pallas_call(
            functools.partial(update_kernel, LEARN_BASE / layers),
            in_specs=[pl.BlockSpec(memory_space=pltpu.VMEM)] * 2 + [pl.BlockSpec(memory_space=pl.ANY)] * 4 +
                     [pl.BlockSpec(memory_space=pltpu.VMEM)],
            out_specs=[pl.BlockSpec(memory_space=pl.ANY)] * 4 + [pl.BlockSpec(memory_space=pltpu.VMEM)] * 2,
            out_shape=[shape((layers, width, hidden), F32), shape((layers, hidden, width), F32),
                       shape((layers, width, hidden), F32), shape((layers, hidden, width), F32),
                       shape((1, rows), F32), shape((rows, width), F32)],
            scratch_shapes=[pltpu.VMEM((SLOTS, width, hidden), F32), pltpu.VMEM((SLOTS, hidden, width), F32),
                            pltpu.VMEM((SLOTS, width, hidden), F32), pltpu.VMEM((SLOTS, hidden, width), F32),
                            pltpu.VMEM((width, hidden), BF16), pltpu.VMEM((hidden, width), BF16),
                            pltpu.VMEM((rows, hidden), BF16),
                            pltpu.SemaphoreType.DMA((SLOTS, 4)), pltpu.SemaphoreType.DMA((SLOTS, 4))],
            compiler_params=pltpu.CompilerParams(vmem_limit_bytes=UPDATE_LIMIT),
            cost_estimate=pl.CostEstimate(flops=2 * matmul_flops, bytes_accessed=160_000_000, transcendentals=0),
            name="update_forward_next",
        )(x_next, y_next, w_first, w_second, m_first, m_second, pltpu.with_memory_space_constraint(grads, pltpu.VMEM))
        return outs[0], outs[1], outs[2], outs[3], outs[4].reshape(rows), outs[5]

    return jax.shard_map(train_step, mesh=mesh,
                         in_specs=(full_spec,) * 4 + (rows_spec,) * 4,
                         out_specs=(full_spec,) * 4 + (P(('pod', 'data')), rows_spec),
                         check_vma=False)
```

```python
import functools

import jax
import jax.numpy as jnp
from jax import lax
from jax.experimental import pallas as pl
from jax.experimental.pallas import tpu as pltpu
from jax.sharding import PartitionSpec as P

LEARN_BASE = 0.25
MOMENTUM = 0.9
C0 = 0.7978845608028654
C1 = C0 * 0.044715
H0, H1 = 2.0 * C0, 8.0 * C1
MESH = pl.DeviceIdType.MESH
F32 = jnp.float32
BF16 = jnp.bfloat16
BACK_LIMIT = 46 << 20
UPDATE_LIMIT = 26 << 20

LOADS = 3
LAGS = (0, 2, 4, 6, 7, 9, 11, 13, 15)
RING = 6
SLOTS = 5
AHEAD = 3


def dot(a, b, ca=1, cb=0):
    return lax.dot_general(a, b, (((ca,), (cb,)), ((), ())), preferred_element_type=F32)


def gelu(half):
    t = jnp.tanh(half * (H0 + H1 * (half * half)))
    return half + half * t


def gelu_both(half):
    sq = half * half
    t = jnp.tanh(half * (H0 + H1 * sq))
    s = 1.0 + t
    u = half * s
    return u, s + u * (1.0 - t) * (H0 + (3.0 * H1) * sq)


def layer_forward(h_ref, w1b_ref, w2b_ref, u_ref, hs_ref, chunk, tile):
    rows, width = h_ref.shape[0], w1b_ref.shape[1]
    for r in range(0, rows, chunk):
        hb = h_ref[r:r + chunk, :].astype(BF16)
        if hs_ref is not None:
            hs_ref[r:r + chunk, :] = hb
        for n in range(0, width, tile):
            u_ref[r:r + chunk, n:n + tile] = gelu(dot(hb, w1b_ref[:, n:n + tile])).astype(BF16)
        h_ref[r:r + chunk, :] = h_ref[r:r + chunk, :] + dot(u_ref[r:r + chunk, :], w2b_ref[...])


def update_kernel(rate, x_ref, y_ref, w1_hbm, w2_hbm, m1_hbm, m2_hbm, gr_ref,
                  w1o_hbm, w2o_hbm, m1o_hbm, m2o_hbm, loss_ref, h_ref,
                  w1_ref, w2_ref, m1_ref, m2_ref, w1b_ref, w2b_ref, u_ref, in_sem, out_sem):
    layers, width = w1_hbm.shape[0], w1_hbm.shape[1]
    states = ((w1_hbm, w1_ref, w1o_hbm), (w2_hbm, w2_ref, w2o_hbm), (m1_hbm, m1_ref, m1o_hbm), (m2_hbm, m2_ref, m2o_hbm))

    def reads(layer):
        slot = layer % SLOTS
        pairs = [(src, buf) for src, buf, _ in states]
        return [pltpu.make_async_copy(src.at[layer], buf.at[slot], in_sem.at[slot, n]) for n, (src, buf) in enumerate(pairs)]

    def writes(layer):
        slot = layer % SLOTS
        return [pltpu.make_async_copy(buf.at[slot], dst.at[layer], out_sem.at[slot, n])
                for n, (_, buf, dst) in enumerate(states)]

    for layer in range(AHEAD):
        for copy in reads(layer):
            copy.start()
    h_ref[...] = x_ref[...].astype(F32)

    @pl.loop(0, layers)
    def _(layer):
        slot = layer % SLOTS

        @pl.when(layer + AHEAD < layers)
        def _():
            @pl.when(layer + AHEAD >= SLOTS)
            def _():
                for copy in writes(layer + AHEAD - SLOTS):
                    copy.wait()
            for copy in reads(layer + AHEAD):
                copy.start()

        for copy in reads(layer):
            copy.wait()
        mom = MOMENTUM * m1_ref[slot] + gr_ref[layer, :width, :].astype(F32)
        m1_ref[slot] = mom
        new = w1_ref[slot] - rate * mom
        w1_ref[slot] = new
        w1b_ref[...] = (0.5 * new).astype(BF16)
        for n in range(0, w2_ref.shape[1], width):
            part = slice(n, n + width)
            mom = MOMENTUM * m2_ref[slot, part, :] + gr_ref[layer, width:, part].astype(F32)
            m2_ref[slot, part, :] = mom
            new = w2_ref[slot, part, :] - rate * mom
            w2_ref[slot, part, :] = new
            w2b_ref[part, :] = new.astype(BF16)
        for copy in writes(layer):
            copy.start()
        layer_forward(h_ref, w1b_ref, w2b_ref, u_ref, None, 512, 256)

    resid = h_ref[...] - y_ref[...].astype(F32)
    loss_ref[...] = jnp.sum((resid * resid).T, axis=0, keepdims=True) / (2 * width)
    for layer in range(layers - SLOTS, layers):
        for copy in writes(layer):
            copy.wait()


def gradient_kernel(scale, x_ref, y_ref, w1f_hbm, w2f_hbm, sum_ref, w1_hbm, w2_hbm, hs_hbm,
                    w1f_buf, w2f_buf, w1_buf, w2_buf, hs_buf, load_sem, save_sem, in_sem, g_ref, gb_ref, gt_ref, ht_ref, u_ref, q_ref,
                    grad_ref, r0_ref, r1_ref, r2_ref, r3_ref, send_sem, recv_sem):
    layers = w1f_hbm.shape[0]
    pod, data = lax.axis_index("pod"), lax.axis_index("data")
    z, y, x, c = pod // 2, pod % 2, data // 2, data % 2
    places = (x, y, z)
    neighbours = ((pod, (1 - x) * 2 + c), (z * 2 + (1 - y), data), ((1 - z) * 2 + y, data))
    sibling = (pod, x * 2 + (1 - c))
    rows, width = g_ref.shape
    hidden = u_ref.shape[1]
    block = 2 * width
    recv_refs = (r0_ref, r1_ref, r2_ref, r3_ref)
    third = hidden // 128 * 3 // 8 * 128
    parts = ((0, third), (third, third), (2 * third, hidden - 2 * third))

    saved = ((w1_hbm, w1_buf), (w2_hbm, w2_buf), (hs_hbm, hs_buf))

    def loads(layer):
        slot = layer % LOADS
        return [pltpu.make_async_copy(src.at[layer], buf.at[slot], load_sem.at[slot, n])
                for n, (src, buf) in enumerate(((w1f_hbm, w1f_buf), (w2f_hbm, w2f_buf)))]

    def saves(layer):
        slot = layer % 2
        return [pltpu.make_async_copy(buf.at[slot], dst.at[layer], save_sem.at[slot, n]) for n, (dst, buf) in enumerate(saved)]

    def reads(layer):
        slot = layer % 2
        return [pltpu.make_async_copy(src.at[layer], buf.at[slot], in_sem.at[slot, n]) for n, (src, buf) in enumerate(saved)]

    for layer in range(LOADS - 1):
        for copy in loads(layer):
            copy.start()
    barrier = pltpu.get_barrier_semaphore()
    for peer in neighbours + (sibling,):
        pl.semaphore_signal(barrier, inc=1, device_id=peer, device_id_type=MESH)
    g_ref[...] = x_ref[...].astype(F32)

    @pl.loop(0, layers)
    def _(layer):
        slot = layer % 2

        @pl.when(layer + LOADS - 1 < layers)
        def _():
            for copy in loads(layer + LOADS - 1):
                copy.start()

        @pl.when(layer >= 2)
        def _():
            for copy in saves(layer - 2):
                copy.wait()

        for copy in loads(layer):
            copy.wait()
        w1_buf[slot] = (0.5 * w1f_buf[layer % LOADS]).astype(BF16)
        w2_buf[slot] = w2f_buf[layer % LOADS].astype(BF16)
        layer_forward(g_ref, w1_buf.at[slot], w2_buf.at[slot], u_ref, hs_buf.at[slot], 1024, 256)

        @pl.when(layer < layers - 2)
        def _():
            for copy in saves(layer):
                copy.start()

    g_ref[...] = (g_ref[...] - y_ref[...].astype(F32)) * scale
    pl.semaphore_wait(barrier, 4)

    def ring(slot):
        return slot % RING

    def context(slot):
        if isinstance(slot, int):
            turn = [(slot + k) % 3 for k in range(3)]
            return slot, slot % RING, [places[k] for k in turn], [neighbours[k] for k in turn]
        start = slot % 3
        first = ((2 - start) * (1 - start) // 2, start * (2 - start), start * (start - 1) // 2)
        turned = [[sum(first[b] * values[(b + k) % 3] for b in range(3)) for k in range(3)]
                  for values in (places, [n[0] for n in neighbours], [n[1] for n in neighbours])]
        return slot, slot % RING, turned[0], list(zip(turned[1], turned[2]))

    def region(ctx, part, stage):
        return sum([ctx[2][(part + n - 1) % 3] * (block >> (n + 1)) for n in range(1, stage + 1)], c * (block // 2))

    def message(ctx, m, part):
        slot, kept, bits, peers = ctx
        if m in (0, 7):
            stage, size, cols, peer = 0, block // 2, slice(None), sibling
            mine, other = c * size, (1 - c) * size
        else:
            stage = m if m <= 3 else 7 - m
            size, cols = block >> (stage + 1), pl.ds(*parts[part])
            axis = (part + stage - 1) % 3
            base, peer = region(ctx, part, stage - 1), peers[axis]
            mine, other = base + bits[axis] * size, base + (1 - bits[axis]) * size
        if m <= 3:
            src = grad_ref.at[kept, pl.ds(pl.multiple_of(other, 16), size), cols]
            dst = recv_refs[stage].at[slot, :, cols]
        else:
            src = sum_ref.at[slot, pl.ds(pl.multiple_of(mine, 16), size), cols]
            dst = src
        return pltpu.make_async_remote_copy(
            src_ref=src, dst_ref=dst, send_sem=send_sem.at[slot, m, part], recv_sem=recv_sem.at[slot, m, part],
            device_id=peer, device_id_type=MESH)

    def parts_of(m):
        return (0,) if m in (0, 7) else (0, 1, 2)

    def accumulate(ctx, stage, part):
        slot, kept = ctx[:2]
        size = block >> (stage + 1)
        if stage == 0:
            mine, cols = c * size, pl.ds(0, hidden)
        else:
            mine, cols = region(ctx, part, stage), pl.ds(*parts[part])
        where = pl.ds(pl.multiple_of(mine, 16), size)
        total = grad_ref[kept, where, cols].astype(F32) + recv_refs[stage][slot, :, cols].astype(F32)
        if stage == 3:
            sum_ref[slot, where, cols] = total.astype(BF16)
        else:
            grad_ref[kept, where, cols] = total.astype(BF16)

    def step(s, slot):
        ctx = context(slot)
        if s > 0:
            m = s - 1
            for part in parts_of(m):
                message(ctx, m, part).wait()
                if m <= 3:
                    accumulate(ctx, m, part)
                if m not in (0, 7) and s < 8 and s != 7:
                    message(ctx, s, part).start()
        if s == 0 or s == 1 or s == 7:
            for part in parts_of(s):
                message(ctx, s, part).start()

    def comm_point(it, parity):
        for s in reversed(range(9)):
            if LAGS[s] % 2 == parity:
                done = it - 1 - (LAGS[s] - parity) // 2

                @pl.when(done >= 0)
                def _():
                    step(s, layers - 1 - done)

    tile, chunk = 256, 256

    @pl.loop(0, layers)
    def _(it):
        comm_point(it, 0)

        layer = layers - 1 - it

        @pl.when((it >= 1) & (it + 1 < layers))
        def _():
            for copy in reads(layer - 1):
                copy.start()

        @pl.when(it >= 2)
        def _():
            for copy in reads(layer):
                copy.wait()

        w1_ref, w2_ref, hs_ref = (buf.at[layer % 2] for buf in (w1_buf, w2_buf, hs_buf))

        gb_ref[...] = g_ref[...].astype(BF16)
        gt_ref[...] = gb_ref[...].T
        ht_ref[...] = hs_ref[...].T

        def first(n, r):
            cols = slice(n, n + tile)
            a = dot(hs_ref[r:r + chunk, :], w1_ref[:, cols])
            gu = dot(gb_ref[r:r + chunk, :], w2_ref[cols, :], 1, 1)
            u, slope = gelu_both(a)
            u_ref[r:r + chunk, cols] = u.astype(BF16)
            q_ref[r:r + chunk, cols] = (slope * gu).astype(BF16)

        def carry(n, r):
            cols = slice(n, n + tile)
            g_ref[r:r + chunk, :] = g_ref[r:r + chunk, :] + dot(q_ref[r:r + chunk, cols], w1_ref[:, cols], 1, 1)

        def grad_second(n):
            cols = slice(n, n + tile)
            grad_ref[ring(layer), width:, cols] = (2.0 * dot(gt_ref[...], u_ref[:, cols])).astype(BF16).T

        def grad_first(n):
            cols = slice(n, n + tile)
            grad_ref[ring(layer), :width, cols] = dot(ht_ref[...], q_ref[:, cols]).astype(BF16)

        def tile_step(n, previous):
            for i, r in enumerate(range(0, rows, chunk)):
                if previous is not None:
                    carry(previous, r)
                    if i == rows // chunk // 2 - 1:
                        grad_second(previous)
                if n is not None:
                    first(n, r)
            if previous is not None:
                grad_first(previous)

        tiles = list(range(0, hidden, tile)) + [None]
        for i, n in enumerate(tiles):
            if i == len(tiles) // 2:
                comm_point(it, 1)
            tile_step(n, tiles[i - 1] if i > 0 else None)

    taken = [sum(2 * n + 2 + lag < 2 * layers for lag in LAGS) for n in range(layers)]
    while min(taken) < 9:
        for n in reversed(range(layers)):
            if taken[n] < 9:
                step(taken[n], layers - 1 - n)
                taken[n] += 1


def solution(mesh):
    n_pod = mesh.shape['pod']
    n_data = mesh.shape['data']
    rows_spec = P(('pod', 'data'), None)
    full_spec = P()

    def train_step(w_first, w_second, m_first, m_second, x_now, y_now, x_next, y_next):
        layers, width, hidden = w_first.shape
        rows = x_now.shape[0]
        batch = rows * n_pod * n_data
        shape = jax.ShapeDtypeStruct
        matmul_flops = 2 * rows * width * hidden * layers

        grads = pl.pallas_call(
            functools.partial(gradient_kernel, 0.5 / (batch * width)),
            in_specs=[pl.BlockSpec(memory_space=pltpu.VMEM)] * 2 + [pl.BlockSpec(memory_space=pl.ANY)] * 2,
            out_specs=[pl.BlockSpec(memory_space=pltpu.VMEM)] + [pl.BlockSpec(memory_space=pl.ANY)] * 3,
            out_shape=[pltpu.VMEM((layers, 2 * width, hidden), BF16), shape((layers - 2, width, hidden), BF16),
                       shape((layers - 2, hidden, width), BF16), shape((layers - 2, rows, width), BF16)],
            scratch_shapes=[
                pltpu.VMEM((LOADS, width, hidden), F32),
                pltpu.VMEM((LOADS, hidden, width), F32),
                pltpu.VMEM((2, width, hidden), BF16),
                pltpu.VMEM((2, hidden, width), BF16),
                pltpu.VMEM((2, rows, width), BF16),
                pltpu.SemaphoreType.DMA((LOADS, 2)),
                pltpu.SemaphoreType.DMA((2, 3)),
                pltpu.SemaphoreType.DMA((2, 3)),
                pltpu.VMEM((rows, width), F32),
                pltpu.VMEM((rows, width), BF16),
                pltpu.VMEM((width, rows), BF16),
                pltpu.VMEM((width, rows), BF16),
                pltpu.VMEM((rows, hidden), BF16),
                pltpu.VMEM((rows, hidden), BF16),
                pltpu.VMEM((RING, 2 * width, hidden), BF16),
                pltpu.VMEM((layers, width, hidden), BF16),
                pltpu.VMEM((layers, width // 2, hidden), BF16),
                pltpu.VMEM((layers, width // 4, hidden), BF16),
                pltpu.VMEM((layers, width // 8, hidden), BF16),
                pltpu.SemaphoreType.DMA((layers, 8, 3)),
                pltpu.SemaphoreType.DMA((layers, 8, 3)),
            ],
            compiler_params=pltpu.CompilerParams(vmem_limit_bytes=BACK_LIMIT,
                                                 collective_id=0, has_side_effects=True),
            cost_estimate=pl.CostEstimate(flops=7 * matmul_flops, bytes_accessed=80_000_000, transcendentals=0),
            name="gradient",
        )(x_now, y_now, w_first, w_second)[0]

        outs = pl.pallas_call(
            functools.partial(update_kernel, LEARN_BASE / layers),
            in_specs=[pl.BlockSpec(memory_space=pltpu.VMEM)] * 2 + [pl.BlockSpec(memory_space=pl.ANY)] * 4 +
                     [pl.BlockSpec(memory_space=pltpu.VMEM)],
            out_specs=[pl.BlockSpec(memory_space=pl.ANY)] * 4 + [pl.BlockSpec(memory_space=pltpu.VMEM)] * 2,
            out_shape=[shape((layers, width, hidden), F32), shape((layers, hidden, width), F32),
                       shape((layers, width, hidden), F32), shape((layers, hidden, width), F32),
                       shape((1, rows), F32), shape((rows, width), F32)],
            scratch_shapes=[pltpu.VMEM((SLOTS, width, hidden), F32), pltpu.VMEM((SLOTS, hidden, width), F32),
                            pltpu.VMEM((SLOTS, width, hidden), F32), pltpu.VMEM((SLOTS, hidden, width), F32),
                            pltpu.VMEM((width, hidden), BF16), pltpu.VMEM((hidden, width), BF16),
                            pltpu.VMEM((rows, hidden), BF16),
                            pltpu.SemaphoreType.DMA((SLOTS, 4)), pltpu.SemaphoreType.DMA((SLOTS, 4))],
            compiler_params=pltpu.CompilerParams(vmem_limit_bytes=UPDATE_LIMIT),
            cost_estimate=pl.CostEstimate(flops=2 * matmul_flops, bytes_accessed=160_000_000, transcendentals=0),
            name="update_forward_next",
        )(x_next, y_next, w_first, w_second, m_first, m_second, pltpu.with_memory_space_constraint(grads, pltpu.VMEM))
        return outs[0], outs[1], outs[2], outs[3], outs[4].reshape(rows), outs[5]

    return jax.shard_map(train_step, mesh=mesh,
                         in_specs=(full_spec,) * 4 + (rows_spec,) * 4,
                         out_specs=(full_spec,) * 4 + (P(('pod', 'data')), rows_spec),
                         check_vma=False)
```

```python
import functools

import jax
import jax.numpy as jnp
from jax import lax
from jax.experimental import pallas as pl
from jax.experimental.pallas import tpu as pltpu
from jax.sharding import PartitionSpec as P

LEARN_BASE = 0.25
MOMENTUM = 0.9
C0 = 0.7978845608028654
C1 = C0 * 0.044715
H0, H1 = 2.0 * C0, 8.0 * C1
MESH = pl.DeviceIdType.MESH
F32 = jnp.float32
BF16 = jnp.bfloat16
BACK_LIMIT = 39 << 20
UPDATE_LIMIT = 31 << 20

KEPT = 2
LAGS = (0, 2, 4, 6, 7, 9, 11, 13, 15)
RING = 6
SLOTS = 5
AHEAD = 3


def dot(a, b, ca=1, cb=0):
    return lax.dot_general(a, b, (((ca,), (cb,)), ((), ())), preferred_element_type=F32)


def gelu(half):
    t = jnp.tanh(half * (H0 + H1 * (half * half)))
    return half + half * t


def gelu_both(half):
    sq = half * half
    t = jnp.tanh(half * (H0 + H1 * sq))
    s = 1.0 + t
    u = half * s
    return u, s + u * (1.0 - t) * (H0 + (3.0 * H1) * sq)


def layer_forward(h_ref, w1b_ref, w2b_ref, u_ref, hs_ref, chunk, tile):
    rows, width = h_ref.shape[0], w1b_ref.shape[1]
    for r in range(0, rows, chunk):
        hb = h_ref[r:r + chunk, :].astype(BF16)
        if hs_ref is not None:
            hs_ref[r:r + chunk, :] = hb
        for n in range(0, width, tile):
            u_ref[r:r + chunk, n:n + tile] = gelu(dot(hb, w1b_ref[:, n:n + tile])).astype(BF16)
        h_ref[r:r + chunk, :] = h_ref[r:r + chunk, :] + dot(u_ref[r:r + chunk, :], w2b_ref[...])


def update_kernel(rate, x_hbm, y_hbm, w1_hbm, w2_hbm, m1_hbm, m2_hbm, k1_ref, k2_ref, gr_ref,
                  w1o_hbm, w2o_hbm, m1o_hbm, m2o_hbm, loss_ref, h_ref,
                  w1_ref, w2_ref, m1_ref, m2_ref, w1b_ref, w2b_ref, u_ref, x_ref, y_ref, in_sem, out_sem, row_sem):
    layers, width = w1_hbm.shape[0], w1_hbm.shape[1]
    states = ((w1_hbm, w1_ref, w1o_hbm), (w2_hbm, w2_ref, w2o_hbm), (m1_hbm, m1_ref, m1o_hbm), (m2_hbm, m2_ref, m2o_hbm))

    def reads(layer):
        slot = layer % SLOTS
        return [pltpu.make_async_copy(src.at[layer], buf.at[slot], in_sem.at[slot, n])
                for n, (src, buf, _) in enumerate(states)]

    def writes(layer):
        slot = layer % SLOTS
        return [pltpu.make_async_copy(buf.at[slot], dst.at[layer], out_sem.at[slot, n])
                for n, (_, buf, dst) in enumerate(states)]

    def refill(layer):
        for copy in writes(layer - SLOTS):
            copy.wait()
        for copy in reads(layer):
            copy.start()

    def advance(layer, w1_old, w2_old, m1_old, m2_old):
        slot = layer % SLOTS
        mom = MOMENTUM * m1_old[...] + gr_ref[layer, :width, :].astype(F32)
        m1_ref[slot] = mom
        new = w1_old[...] - rate * mom
        w1_ref[slot] = new
        w1b_ref[...] = (0.5 * new).astype(BF16)
        for n in range(0, w2_ref.shape[1], width):
            part = slice(n, n + width)
            mom = MOMENTUM * m2_old[part, :] + gr_ref[layer, width:, part].astype(F32)
            m2_ref[slot, part, :] = mom
            new = w2_old[part, :] - rate * mom
            w2_ref[slot, part, :] = new
            w2b_ref[part, :] = new.astype(BF16)
        for copy in writes(layer):
            copy.start()
        layer_forward(h_ref, w1b_ref, w2b_ref, u_ref, None, 512, 256)

    x_copy = pltpu.make_async_copy(x_hbm, x_ref, row_sem.at[0])
    y_copy = pltpu.make_async_copy(y_hbm, y_ref, row_sem.at[1])
    x_copy.start()
    for layer in range(KEPT, SLOTS):
        for copy in reads(layer):
            copy.start()
    y_copy.start()
    x_copy.wait()
    h_ref[...] = x_ref[...].astype(F32)
    for layer in range(KEPT):
        if layer + AHEAD >= SLOTS:
            refill(layer + AHEAD)
        advance(layer, *(ref.at[start + layer] for start in (0, KEPT) for ref in (k1_ref, k2_ref)))

    @pl.loop(KEPT, layers)
    def _(layer):
        @pl.when(layer + AHEAD < layers)
        def _():
            refill(layer + AHEAD)

        for copy in reads(layer):
            copy.wait()
        advance(layer, *(buf.at[layer % SLOTS] for _, buf, _ in states))

    y_copy.wait()
    resid = h_ref[...] - y_ref[...].astype(F32)
    loss_ref[...] = jnp.sum((resid * resid).T, axis=0, keepdims=True) / (2 * width)
    for layer in range(layers - SLOTS, layers):
        for copy in writes(layer):
            copy.wait()


def gradient_kernel(scale, x_ref, y_ref, w1f_hbm, w2f_hbm, m1f_hbm, m2f_hbm,
                    k1_ref, k2_ref, sum_ref, w1_hbm, w2_hbm, hs_hbm, w1_buf, w2_buf, hs_buf, load_sem, save_sem, in_sem, keep_sem, g_ref, gb_ref, gt_ref, ht_ref, u_ref, q_ref,
                    grad_ref, r0_ref, r1_ref, r2_ref, r3_ref, send_sem, recv_sem):
    layers = w1f_hbm.shape[0]
    w1f_buf, m1f_buf, w2f_buf, m2f_buf = (ref.at[pl.ds(start, KEPT)] for ref in (k1_ref, k2_ref) for start in (0, KEPT))
    pod, data = lax.axis_index("pod"), lax.axis_index("data")
    z, y, x, c = pod // 2, pod % 2, data // 2, data % 2
    places = (x, y, z)
    neighbours = ((pod, (1 - x) * 2 + c), (z * 2 + (1 - y), data), ((1 - z) * 2 + y, data))
    sibling = (pod, x * 2 + (1 - c))
    rows, width = g_ref.shape
    hidden = u_ref.shape[1]
    block = 2 * width
    recv_refs = (r0_ref, r1_ref, r2_ref, r3_ref)
    third = hidden // 128 * 3 // 8 * 128
    parts = ((0, third), (third, third), (2 * third, hidden - 2 * third))

    saved = ((w1_hbm, w1_buf), (w2_hbm, w2_buf), (hs_hbm, hs_buf))

    def loads(layer):
        slot = layer % KEPT
        return [pltpu.make_async_copy(src.at[layer], buf.at[slot], load_sem.at[slot, n])
                for n, (src, buf) in enumerate(((w1f_hbm, w1f_buf), (w2f_hbm, w2f_buf)))]

    def saves(layer):
        slot = layer % 2
        return [pltpu.make_async_copy(buf.at[slot], dst.at[layer], save_sem.at[slot, n]) for n, (dst, buf) in enumerate(saved)]

    def reads(layer):
        slot = layer % 2
        return [pltpu.make_async_copy(src.at[layer], buf.at[slot], in_sem.at[slot, n]) for n, (src, buf) in enumerate(saved)]

    keeps = [pltpu.make_async_copy(src.at[pl.ds(0, KEPT)], buf, keep_sem.at[n]) for n, (src, buf) in enumerate(
        ((w1f_hbm, w1f_buf), (w2f_hbm, w2f_buf), (m1f_hbm, m1f_buf), (m2f_hbm, m2f_buf)))]

    for layer in range(KEPT - 1):
        for copy in loads(layer):
            copy.start()
    barrier = pltpu.get_barrier_semaphore()
    for peer in neighbours + (sibling,):
        pl.semaphore_signal(barrier, inc=1, device_id=peer, device_id_type=MESH)
    g_ref[...] = x_ref[...].astype(F32)

    @pl.loop(0, layers)
    def _(layer):
        slot = layer % 2

        @pl.when(layer + KEPT - 1 < layers)
        def _():
            for copy in loads(layer + KEPT - 1):
                copy.start()

        @pl.when(layer >= 2)
        def _():
            for copy in saves(layer - 2):
                copy.wait()

        for copy in loads(layer):
            copy.wait()
        w1_buf[slot] = (0.5 * w1f_buf[layer % KEPT]).astype(BF16)
        w2_buf[slot] = w2f_buf[layer % KEPT].astype(BF16)
        layer_forward(g_ref, w1_buf.at[slot], w2_buf.at[slot], u_ref, hs_buf.at[slot], 1024, 256)

        @pl.when(layer < layers - 2)
        def _():
            for copy in saves(layer):
                copy.start()

    g_ref[...] = (g_ref[...] - y_ref[...].astype(F32)) * scale
    for copy in keeps:
        copy.start()
    pl.semaphore_wait(barrier, 4)

    def ring(slot):
        return slot % RING

    def context(slot):
        if isinstance(slot, int):
            turn = [(slot + k) % 3 for k in range(3)]
            return slot, slot % RING, [places[k] for k in turn], [neighbours[k] for k in turn]
        start = slot % 3
        first = ((2 - start) * (1 - start) // 2, start * (2 - start), start * (start - 1) // 2)
        turned = [[sum(first[b] * values[(b + k) % 3] for b in range(3)) for k in range(3)]
                  for values in (places, [n[0] for n in neighbours], [n[1] for n in neighbours])]
        return slot, slot % RING, turned[0], list(zip(turned[1], turned[2]))

    def region(ctx, part, stage):
        return sum([ctx[2][(part + n - 1) % 3] * (block >> (n + 1)) for n in range(1, stage + 1)], c * (block // 2))

    def message(ctx, m, part):
        slot, kept, bits, peers = ctx
        if m in (0, 7):
            stage, size, cols, peer = 0, block // 2, slice(None), sibling
            mine, other = c * size, (1 - c) * size
        else:
            stage = m if m <= 3 else 7 - m
            size, cols = block >> (stage + 1), pl.ds(*parts[part])
            axis = (part + stage - 1) % 3
            base, peer = region(ctx, part, stage - 1), peers[axis]
            mine, other = base + bits[axis] * size, base + (1 - bits[axis]) * size
        if m <= 3:
            src = grad_ref.at[kept, pl.ds(pl.multiple_of(other, 16), size), cols]
            dst = recv_refs[stage].at[slot, :, cols]
        else:
            src = sum_ref.at[slot, pl.ds(pl.multiple_of(mine, 16), size), cols]
            dst = src
        return pltpu.make_async_remote_copy(
            src_ref=src, dst_ref=dst, send_sem=send_sem.at[slot, m, part], recv_sem=recv_sem.at[slot, m, part],
            device_id=peer, device_id_type=MESH)

    def parts_of(m):
        return (0,) if m in (0, 7) else (0, 1, 2)

    def accumulate(ctx, stage, part):
        slot, kept = ctx[:2]
        size = block >> (stage + 1)
        if stage == 0:
            mine, cols = c * size, pl.ds(0, hidden)
        else:
            mine, cols = region(ctx, part, stage), pl.ds(*parts[part])
        where = pl.ds(pl.multiple_of(mine, 16), size)
        total = grad_ref[kept, where, cols].astype(F32) + recv_refs[stage][slot, :, cols].astype(F32)
        if stage == 3:
            sum_ref[slot, where, cols] = total.astype(BF16)
        else:
            grad_ref[kept, where, cols] = total.astype(BF16)

    def step(s, slot):
        ctx = context(slot)
        if s > 0:
            m = s - 1
            for part in parts_of(m):
                message(ctx, m, part).wait()
                if m <= 3:
                    accumulate(ctx, m, part)
                if m not in (0, 7) and s < 8 and s != 7:
                    message(ctx, s, part).start()
        if s == 0 or s == 1 or s == 7:
            for part in parts_of(s):
                message(ctx, s, part).start()

    def comm_point(it, parity):
        for s in reversed(range(9)):
            if LAGS[s] % 2 == parity:
                done = it - 1 - (LAGS[s] - parity) // 2

                @pl.when(done >= 0)
                def _():
                    step(s, layers - 1 - done)

    tile, chunk = 256, 256

    @pl.loop(0, layers)
    def _(it):
        comm_point(it, 0)

        layer = layers - 1 - it

        @pl.when((it >= 1) & (it + 1 < layers))
        def _():
            for copy in reads(layer - 1):
                copy.start()

        @pl.when(it >= 2)
        def _():
            for copy in reads(layer):
                copy.wait()

        w1_ref, w2_ref, hs_ref = (buf.at[layer % 2] for buf in (w1_buf, w2_buf, hs_buf))

        gb_ref[...] = g_ref[...].astype(BF16)
        gt_ref[...] = gb_ref[...].T
        ht_ref[...] = hs_ref[...].T

        def first(n, r):
            cols = slice(n, n + tile)
            a = dot(hs_ref[r:r + chunk, :], w1_ref[:, cols])
            gu = dot(gb_ref[r:r + chunk, :], w2_ref[cols, :], 1, 1)
            u, slope = gelu_both(a)
            u_ref[r:r + chunk, cols] = u.astype(BF16)
            q_ref[r:r + chunk, cols] = (slope * gu).astype(BF16)

        def carry(n, r):
            cols = slice(n, n + tile)
            g_ref[r:r + chunk, :] = g_ref[r:r + chunk, :] + dot(q_ref[r:r + chunk, cols], w1_ref[:, cols], 1, 1)

        def grad_second(n):
            cols = slice(n, n + tile)
            grad_ref[ring(layer), width:, cols] = (2.0 * dot(gt_ref[...], u_ref[:, cols])).astype(BF16).T

        def grad_first(n):
            cols = slice(n, n + tile)
            grad_ref[ring(layer), :width, cols] = dot(ht_ref[...], q_ref[:, cols]).astype(BF16)

        def tile_step(n, previous):
            for i, r in enumerate(range(0, rows, chunk)):
                if previous is not None:
                    carry(previous, r)
                    if i == rows // chunk // 2 - 1:
                        grad_second(previous)
                if n is not None:
                    first(n, r)
            if previous is not None:
                grad_first(previous)

        tiles = list(range(0, hidden, tile)) + [None]
        for i, n in enumerate(tiles):
            if i == len(tiles) // 2:
                comm_point(it, 1)
            tile_step(n, tiles[i - 1] if i > 0 else None)

    taken = [sum(2 * n + 2 + lag < 2 * layers for lag in LAGS) for n in range(layers)]
    while min(taken) < 9:
        for n in reversed(range(layers)):
            if taken[n] < 9:
                step(taken[n], layers - 1 - n)
                taken[n] += 1
    for copy in keeps:
        copy.wait()


def solution(mesh):
    n_pod = mesh.shape['pod']
    n_data = mesh.shape['data']
    rows_spec = P(('pod', 'data'), None)
    full_spec = P()

    def train_step(w_first, w_second, m_first, m_second, x_now, y_now, x_next, y_next):
        layers, width, hidden = w_first.shape
        rows = x_now.shape[0]
        batch = rows * n_pod * n_data
        shape = jax.ShapeDtypeStruct
        matmul_flops = 2 * rows * width * hidden * layers

        kept = pl.pallas_call(
            functools.partial(gradient_kernel, 0.5 / (batch * width)),
            in_specs=[pl.BlockSpec(memory_space=pltpu.VMEM)] * 2 + [pl.BlockSpec(memory_space=pl.ANY)] * 4,
            out_specs=[pl.BlockSpec(memory_space=pltpu.VMEM)] * 3 + [pl.BlockSpec(memory_space=pl.ANY)] * 3,
            out_shape=[pltpu.VMEM((2 * KEPT, width, hidden), F32), pltpu.VMEM((2 * KEPT, hidden, width), F32),
                       pltpu.VMEM((layers, 2 * width, hidden), BF16),
                       shape((layers - 2, width, hidden), BF16),
                       shape((layers - 2, hidden, width), BF16), shape((layers - 2, rows, width), BF16)],
            scratch_shapes=[
                pltpu.VMEM((2, width, hidden), BF16),
                pltpu.VMEM((2, hidden, width), BF16),
                pltpu.VMEM((2, rows, width), BF16),
                pltpu.SemaphoreType.DMA((KEPT, 2)),
                pltpu.SemaphoreType.DMA((2, 3)),
                pltpu.SemaphoreType.DMA((2, 3)),
                pltpu.SemaphoreType.DMA((4,)),
                pltpu.VMEM((rows, width), F32),
                pltpu.VMEM((rows, width), BF16),
                pltpu.VMEM((width, rows), BF16),
                pltpu.VMEM((width, rows), BF16),
                pltpu.VMEM((rows, hidden), BF16),
                pltpu.VMEM((rows, hidden), BF16),
                pltpu.VMEM((RING, 2 * width, hidden), BF16),
                pltpu.VMEM((layers, width, hidden), BF16),
                pltpu.VMEM((layers, width // 2, hidden), BF16),
                pltpu.VMEM((layers, width // 4, hidden), BF16),
                pltpu.VMEM((layers, width // 8, hidden), BF16),
                pltpu.SemaphoreType.DMA((layers, 8, 3)),
                pltpu.SemaphoreType.DMA((layers, 8, 3)),
            ],
            compiler_params=pltpu.CompilerParams(vmem_limit_bytes=BACK_LIMIT,
                                                 collective_id=0, has_side_effects=True),
            cost_estimate=pl.CostEstimate(flops=7 * matmul_flops, bytes_accessed=80_000_000, transcendentals=0),
            name="gradient",
        )(x_now, y_now, w_first, w_second, m_first, m_second)[:3]

        outs = pl.pallas_call(
            functools.partial(update_kernel, LEARN_BASE / layers),
            in_specs=[pl.BlockSpec(memory_space=pl.ANY)] * 6 +
                     [pl.BlockSpec(memory_space=pltpu.VMEM)] * 3,
            out_specs=[pl.BlockSpec(memory_space=pl.ANY)] * 4 + [pl.BlockSpec(memory_space=pltpu.VMEM)] * 2,
            out_shape=[shape((layers, width, hidden), F32), shape((layers, hidden, width), F32),
                       shape((layers, width, hidden), F32), shape((layers, hidden, width), F32),
                       shape((1, rows), F32), shape((rows, width), F32)],
            scratch_shapes=[pltpu.VMEM((SLOTS, width, hidden), F32), pltpu.VMEM((SLOTS, hidden, width), F32),
                            pltpu.VMEM((SLOTS, width, hidden), F32), pltpu.VMEM((SLOTS, hidden, width), F32),
                            pltpu.VMEM((width, hidden), BF16), pltpu.VMEM((hidden, width), BF16),
                            pltpu.VMEM((rows, hidden), BF16),
                            pltpu.VMEM((rows, width), BF16), pltpu.VMEM((rows, width), BF16),
                            pltpu.SemaphoreType.DMA((SLOTS, 4)), pltpu.SemaphoreType.DMA((SLOTS, 4)),
                            pltpu.SemaphoreType.DMA((2,))],
            compiler_params=pltpu.CompilerParams(vmem_limit_bytes=UPDATE_LIMIT),
            cost_estimate=pl.CostEstimate(flops=2 * matmul_flops, bytes_accessed=160_000_000, transcendentals=0),
            name="update_forward_next",
        )(*(pltpu.with_memory_space_constraint(a, pltpu.HBM) for a in (x_next, y_next)), w_first, w_second, m_first, m_second,
          *(pltpu.with_memory_space_constraint(a, pltpu.VMEM) for a in kept))
        return outs[0], outs[1], outs[2], outs[3], outs[4].reshape(rows), outs[5]

    return jax.shard_map(train_step, mesh=mesh,
                         in_specs=(full_spec,) * 4 + (rows_spec,) * 4,
                         out_specs=(full_spec,) * 4 + (P(('pod', 'data')), rows_spec),
                         check_vma=False)
```

```python
import functools

import jax
import jax.numpy as jnp
from jax import lax
from jax.experimental import pallas as pl
from jax.experimental.pallas import tpu as pltpu
from jax.sharding import PartitionSpec as P

LEARN_BASE = 0.25
MOMENTUM = 0.9
C0 = 0.7978845608028654
C1 = C0 * 0.044715
H0, H1 = 2.0 * C0, 8.0 * C1
MESH = pl.DeviceIdType.MESH
F32 = jnp.float32
BF16 = jnp.bfloat16
BACK_LIMIT = 46 << 20
UPDATE_LIMIT = 30 << 20

LOADS = 3
LAGS = (0, 2, 4, 6, 7, 9, 11, 13, 15)
RING = 6
SLOTS = 6
AHEAD = 4


def dot(a, b, ca=1, cb=0):
    return lax.dot_general(a, b, (((ca,), (cb,)), ((), ())), preferred_element_type=F32)


def gelu(half):
    t = jnp.tanh(half * (H0 + H1 * (half * half)))
    return half + half * t


def gelu_both(half):
    sq = half * half
    t = jnp.tanh(half * (H0 + H1 * sq))
    s = 1.0 + t
    u = half * s
    return u, s + u * (1.0 - t) * (H0 + (3.0 * H1) * sq)


def layer_forward(h_ref, w1b_ref, w2b_ref, u_ref, hs_ref, chunk, tile):
    rows, width = h_ref.shape[0], w1b_ref.shape[1]
    for r in range(0, rows, chunk):
        hb = h_ref[r:r + chunk, :].astype(BF16)
        if hs_ref is not None:
            hs_ref[r:r + chunk, :] = hb
        for n in range(0, width, tile):
            u_ref[r:r + chunk, n:n + tile] = gelu(dot(hb, w1b_ref[:, n:n + tile])).astype(BF16)
        h_ref[r:r + chunk, :] = h_ref[r:r + chunk, :] + dot(u_ref[r:r + chunk, :], w2b_ref[...])


def update_kernel(rate, x_ref, y_ref, w1_hbm, w2_hbm, m1_hbm, m2_hbm, gr_ref,
                  w1o_hbm, w2o_hbm, m1o_hbm, m2o_hbm, loss_ref, h_ref,
                  w1_ref, w2_ref, m1_ref, m2_ref, w1b_ref, w2b_ref, u_ref, in_sem, out_sem):
    layers, width = w1_hbm.shape[0], w1_hbm.shape[1]
    states = ((w1_hbm, w1_ref, w1o_hbm), (w2_hbm, w2_ref, w2o_hbm), (m1_hbm, m1_ref, m1o_hbm), (m2_hbm, m2_ref, m2o_hbm))

    def reads(layer):
        slot = layer % SLOTS
        pairs = [(src, buf) for src, buf, _ in states]
        return [pltpu.make_async_copy(src.at[layer], buf.at[slot], in_sem.at[slot, n]) for n, (src, buf) in enumerate(pairs)]

    def writes(layer):
        slot = layer % SLOTS
        return [pltpu.make_async_copy(buf.at[slot], dst.at[layer], out_sem.at[slot, n])
                for n, (_, buf, dst) in enumerate(states)]

    for layer in range(AHEAD):
        for copy in reads(layer):
            copy.start()
    h_ref[...] = x_ref[...].astype(F32)

    @pl.loop(0, layers)
    def _(layer):
        slot = layer % SLOTS

        @pl.when(layer + AHEAD < layers)
        def _():
            @pl.when(layer + AHEAD >= SLOTS)
            def _():
                for copy in writes(layer + AHEAD - SLOTS):
                    copy.wait()
            for copy in reads(layer + AHEAD):
                copy.start()

        for copy in reads(layer):
            copy.wait()
        mom = MOMENTUM * m1_ref[slot] + gr_ref[layer, :width, :].astype(F32)
        m1_ref[slot] = mom
        new = w1_ref[slot] - rate * mom
        w1_ref[slot] = new
        w1b_ref[...] = (0.5 * new).astype(BF16)
        for n in range(0, w2_ref.shape[1], width):
            part = slice(n, n + width)
            mom = MOMENTUM * m2_ref[slot, part, :] + gr_ref[layer, width:, part].astype(F32)
            m2_ref[slot, part, :] = mom
            new = w2_ref[slot, part, :] - rate * mom
            w2_ref[slot, part, :] = new
            w2b_ref[part, :] = new.astype(BF16)
        for copy in writes(layer):
            copy.start()
        layer_forward(h_ref, w1b_ref, w2b_ref, u_ref, None, 1024, 256)

    resid = h_ref[...] - y_ref[...].astype(F32)
    loss_ref[...] = jnp.sum((resid * resid).T, axis=0, keepdims=True) / (2 * width)
    for layer in range(layers - SLOTS, layers):
        for copy in writes(layer):
            copy.wait()


def gradient_kernel(scale, x_ref, y_ref, w1f_hbm, w2f_hbm, sum_ref, w1_hbm, w2_hbm, hs_hbm,
                    w1f_buf, w2f_buf, w1_buf, w2_buf, hs_buf, load_sem, save_sem, in_sem, g_ref, gb_ref, gt_ref, ht_ref, u_ref, q_ref,
                    grad_ref, r0_ref, r1_ref, r2_ref, r3_ref, send_sem, recv_sem):
    layers = w1f_hbm.shape[0]
    pod, data = lax.axis_index("pod"), lax.axis_index("data")
    z, y, x, c = pod // 2, pod % 2, data // 2, data % 2
    places = (x, y, z)
    neighbours = ((pod, (1 - x) * 2 + c), (z * 2 + (1 - y), data), ((1 - z) * 2 + y, data))
    sibling = (pod, x * 2 + (1 - c))
    rows, width = g_ref.shape
    hidden = u_ref.shape[1]
    block = 2 * width
    recv_refs = (r0_ref, r1_ref, r2_ref, r3_ref)
    third = hidden // 128 * 3 // 8 * 128
    parts = ((0, third), (third, third), (2 * third, hidden - 2 * third))

    saved = ((w1_hbm, w1_buf), (w2_hbm, w2_buf), (hs_hbm, hs_buf))

    def loads(layer):
        slot = layer % LOADS
        return [pltpu.make_async_copy(src.at[layer], buf.at[slot], load_sem.at[slot, n])
                for n, (src, buf) in enumerate(((w1f_hbm, w1f_buf), (w2f_hbm, w2f_buf)))]

    def saves(layer):
        slot = layer % 2
        return [pltpu.make_async_copy(buf.at[slot], dst.at[layer], save_sem.at[slot, n]) for n, (dst, buf) in enumerate(saved)]

    def reads(layer):
        slot = layer % 2
        return [pltpu.make_async_copy(src.at[layer], buf.at[slot], in_sem.at[slot, n]) for n, (src, buf) in enumerate(saved)]

    for layer in range(LOADS - 1):
        for copy in loads(layer):
            copy.start()
    barrier = pltpu.get_barrier_semaphore()
    for peer in neighbours + (sibling,):
        pl.semaphore_signal(barrier, inc=1, device_id=peer, device_id_type=MESH)
    g_ref[...] = x_ref[...].astype(F32)

    @pl.loop(0, layers)
    def _(layer):
        slot = layer % 2

        @pl.when(layer + LOADS - 1 < layers)
        def _():
            for copy in loads(layer + LOADS - 1):
                copy.start()

        @pl.when(layer >= 2)
        def _():
            for copy in saves(layer - 2):
                copy.wait()

        for copy in loads(layer):
            copy.wait()
        w1_buf[slot] = (0.5 * w1f_buf[layer % LOADS]).astype(BF16)
        w2_buf[slot] = w2f_buf[layer % LOADS].astype(BF16)
        layer_forward(g_ref, w1_buf.at[slot], w2_buf.at[slot], u_ref, hs_buf.at[slot], 1024, 256)

        @pl.when(layer < layers - 2)
        def _():
            for copy in saves(layer):
                copy.start()

    g_ref[...] = (g_ref[...] - y_ref[...].astype(F32)) * scale
    pl.semaphore_wait(barrier, 4)

    def ring(slot):
        return slot % RING

    def context(slot):
        if isinstance(slot, int):
            turn = [(slot + k) % 3 for k in range(3)]
            return slot, slot % RING, [places[k] for k in turn], [neighbours[k] for k in turn]
        start = slot % 3
        first = ((2 - start) * (1 - start) // 2, start * (2 - start), start * (start - 1) // 2)
        turned = [[sum(first[b] * values[(b + k) % 3] for b in range(3)) for k in range(3)]
                  for values in (places, [n[0] for n in neighbours], [n[1] for n in neighbours])]
        return slot, slot % RING, turned[0], list(zip(turned[1], turned[2]))

    def region(ctx, part, stage):
        return sum([ctx[2][(part + n - 1) % 3] * (block >> (n + 1)) for n in range(1, stage + 1)], c * (block // 2))

    def message(ctx, m, part):
        slot, kept, bits, peers = ctx
        if m in (0, 7):
            stage, size, cols, peer = 0, block // 2, slice(None), sibling
            mine, other = c * size, (1 - c) * size
        else:
            stage = m if m <= 3 else 7 - m
            size, cols = block >> (stage + 1), pl.ds(*parts[part])
            axis = (part + stage - 1) % 3
            base, peer = region(ctx, part, stage - 1), peers[axis]
            mine, other = base + bits[axis] * size, base + (1 - bits[axis]) * size
        if m <= 3:
            src = grad_ref.at[kept, pl.ds(pl.multiple_of(other, 16), size), cols]
            dst = recv_refs[stage].at[slot, :, cols]
        else:
            src = sum_ref.at[slot, pl.ds(pl.multiple_of(mine, 16), size), cols]
            dst = src
        return pltpu.make_async_remote_copy(
            src_ref=src, dst_ref=dst, send_sem=send_sem.at[slot, m, part], recv_sem=recv_sem.at[slot, m, part],
            device_id=peer, device_id_type=MESH)

    def parts_of(m):
        return (0,) if m in (0, 7) else (0, 1, 2)

    def accumulate(ctx, stage, part):
        slot, kept = ctx[:2]
        size = block >> (stage + 1)
        if stage == 0:
            mine, cols = c * size, pl.ds(0, hidden)
        else:
            mine, cols = region(ctx, part, stage), pl.ds(*parts[part])
        where = pl.ds(pl.multiple_of(mine, 16), size)
        total = grad_ref[kept, where, cols].astype(F32) + recv_refs[stage][slot, :, cols].astype(F32)
        if stage == 3:
            sum_ref[slot, where, cols] = total.astype(BF16)
        else:
            grad_ref[kept, where, cols] = total.astype(BF16)

    def step(s, slot):
        ctx = context(slot)
        if s > 0:
            m = s - 1
            for part in parts_of(m):
                message(ctx, m, part).wait()
                if m <= 3:
                    accumulate(ctx, m, part)
                if m not in (0, 7) and s < 8 and s != 7:
                    message(ctx, s, part).start()
        if s == 0 or s == 1 or s == 7:
            for part in parts_of(s):
                message(ctx, s, part).start()

    def comm_point(it, parity):
        for s in reversed(range(9)):
            if LAGS[s] % 2 == parity:
                done = it - 1 - (LAGS[s] - parity) // 2

                @pl.when(done >= 0)
                def _():
                    step(s, layers - 1 - done)

    tile, chunk = 256, 256

    @pl.loop(0, layers)
    def _(it):
        comm_point(it, 0)

        layer = layers - 1 - it

        @pl.when((it >= 1) & (it + 1 < layers))
        def _():
            for copy in reads(layer - 1):
                copy.start()

        @pl.when(it >= 2)
        def _():
            for copy in reads(layer):
                copy.wait()

        w1_ref, w2_ref, hs_ref = (buf.at[layer % 2] for buf in (w1_buf, w2_buf, hs_buf))

        gb_ref[...] = g_ref[...].astype(BF16)
        gt_ref[...] = gb_ref[...].T
        ht_ref[...] = hs_ref[...].T

        def first(n, r):
            cols = slice(n, n + tile)
            a = dot(hs_ref[r:r + chunk, :], w1_ref[:, cols])
            gu = dot(gb_ref[r:r + chunk, :], w2_ref[cols, :], 1, 1)
            u, slope = gelu_both(a)
            u_ref[r:r + chunk, cols] = u.astype(BF16)
            q_ref[r:r + chunk, cols] = (slope * gu).astype(BF16)

        def carry(n, r):
            cols = slice(n, n + tile)
            g_ref[r:r + chunk, :] = g_ref[r:r + chunk, :] + dot(q_ref[r:r + chunk, cols], w1_ref[:, cols], 1, 1)

        def grad_second(n):
            cols = slice(n, n + tile)
            grad_ref[ring(layer), width:, cols] = (2.0 * dot(gt_ref[...], u_ref[:, cols])).astype(BF16).T

        def grad_first(n):
            cols = slice(n, n + tile)
            grad_ref[ring(layer), :width, cols] = dot(ht_ref[...], q_ref[:, cols]).astype(BF16)

        def tile_step(n, previous):
            for i, r in enumerate(range(0, rows, chunk)):
                if previous is not None:
                    carry(previous, r)
                    if i == rows // chunk // 2 - 1:
                        grad_second(previous)
                if n is not None:
                    first(n, r)
            if previous is not None:
                grad_first(previous)

        tiles = list(range(0, hidden, tile)) + [None]
        for i, n in enumerate(tiles):
            if i == len(tiles) // 2:
                comm_point(it, 1)
            tile_step(n, tiles[i - 1] if i > 0 else None)

    taken = [sum(2 * n + 2 + lag < 2 * layers for lag in LAGS) for n in range(layers)]
    while min(taken) < 9:
        for n in reversed(range(layers)):
            if taken[n] < 9:
                step(taken[n], layers - 1 - n)
                taken[n] += 1


def solution(mesh):
    n_pod = mesh.shape['pod']
    n_data = mesh.shape['data']
    rows_spec = P(('pod', 'data'), None)
    full_spec = P()

    def train_step(w_first, w_second, m_first, m_second, x_now, y_now, x_next, y_next):
        layers, width, hidden = w_first.shape
        rows = x_now.shape[0]
        batch = rows * n_pod * n_data
        shape = jax.ShapeDtypeStruct
        matmul_flops = 2 * rows * width * hidden * layers

        grads = pl.pallas_call(
            functools.partial(gradient_kernel, 0.5 / (batch * width)),
            in_specs=[pl.BlockSpec(memory_space=pltpu.VMEM)] * 2 + [pl.BlockSpec(memory_space=pl.ANY)] * 2,
            out_specs=[pl.BlockSpec(memory_space=pltpu.VMEM)] + [pl.BlockSpec(memory_space=pl.ANY)] * 3,
            out_shape=[pltpu.VMEM((layers, 2 * width, hidden), BF16), shape((layers - 2, width, hidden), BF16),
                       shape((layers - 2, hidden, width), BF16), shape((layers - 2, rows, width), BF16)],
            scratch_shapes=[
                pltpu.VMEM((LOADS, width, hidden), F32),
                pltpu.VMEM((LOADS, hidden, width), F32),
                pltpu.VMEM((2, width, hidden), BF16),
                pltpu.VMEM((2, hidden, width), BF16),
                pltpu.VMEM((2, rows, width), BF16),
                pltpu.SemaphoreType.DMA((LOADS, 2)),
                pltpu.SemaphoreType.DMA((2, 3)),
                pltpu.SemaphoreType.DMA((2, 3)),
                pltpu.VMEM((rows, width), F32),
                pltpu.VMEM((rows, width), BF16),
                pltpu.VMEM((width, rows), BF16),
                pltpu.VMEM((width, rows), BF16),
                pltpu.VMEM((rows, hidden), BF16),
                pltpu.VMEM((rows, hidden), BF16),
                pltpu.VMEM((RING, 2 * width, hidden), BF16),
                pltpu.VMEM((layers, width, hidden), BF16),
                pltpu.VMEM((layers, width // 2, hidden), BF16),
                pltpu.VMEM((layers, width // 4, hidden), BF16),
                pltpu.VMEM((layers, width // 8, hidden), BF16),
                pltpu.SemaphoreType.DMA((layers, 8, 3)),
                pltpu.SemaphoreType.DMA((layers, 8, 3)),
            ],
            compiler_params=pltpu.CompilerParams(vmem_limit_bytes=BACK_LIMIT,
                                                 collective_id=0, has_side_effects=True),
            cost_estimate=pl.CostEstimate(flops=7 * matmul_flops, bytes_accessed=80_000_000, transcendentals=0),
            name="gradient",
        )(x_now, y_now, w_first, w_second)[0]

        outs = pl.pallas_call(
            functools.partial(update_kernel, LEARN_BASE / layers),
            in_specs=[pl.BlockSpec(memory_space=pltpu.VMEM)] * 2 + [pl.BlockSpec(memory_space=pl.ANY)] * 4 +
                     [pl.BlockSpec(memory_space=pltpu.VMEM)],
            out_specs=[pl.BlockSpec(memory_space=pl.ANY)] * 4 + [pl.BlockSpec(memory_space=pltpu.VMEM)] * 2,
            out_shape=[shape((layers, width, hidden), F32), shape((layers, hidden, width), F32),
                       shape((layers, width, hidden), F32), shape((layers, hidden, width), F32),
                       shape((1, rows), F32), shape((rows, width), F32)],
            scratch_shapes=[pltpu.VMEM((SLOTS, width, hidden), F32), pltpu.VMEM((SLOTS, hidden, width), F32),
                            pltpu.VMEM((SLOTS, width, hidden), F32), pltpu.VMEM((SLOTS, hidden, width), F32),
                            pltpu.VMEM((width, hidden), BF16), pltpu.VMEM((hidden, width), BF16),
                            pltpu.VMEM((rows, hidden), BF16),
                            pltpu.SemaphoreType.DMA((SLOTS, 4)), pltpu.SemaphoreType.DMA((SLOTS, 4))],
            compiler_params=pltpu.CompilerParams(vmem_limit_bytes=UPDATE_LIMIT),
            cost_estimate=pl.CostEstimate(flops=2 * matmul_flops, bytes_accessed=160_000_000, transcendentals=0),
            name="update_forward_next",
        )(x_next, y_next, w_first, w_second, m_first, m_second, pltpu.with_memory_space_constraint(grads, pltpu.VMEM))
        return outs[0], outs[1], outs[2], outs[3], outs[4].reshape(rows), outs[5]

    return jax.shard_map(train_step, mesh=mesh,
                         in_specs=(full_spec,) * 4 + (rows_spec,) * 4,
                         out_specs=(full_spec,) * 4 + (P(('pod', 'data')), rows_spec),
                         check_vma=False)
```

```python
import functools

import jax
import jax.numpy as jnp
from jax import lax
from jax.experimental import pallas as pl
from jax.experimental.pallas import tpu as pltpu
from jax.sharding import PartitionSpec as P

LEARN_BASE = 0.25
MOMENTUM = 0.9
C0 = 0.7978845608028654
C1 = C0 * 0.044715
H0, H1 = 2.0 * C0, 8.0 * C1
MESH = pl.DeviceIdType.MESH
F32 = jnp.float32
BF16 = jnp.bfloat16
BACK_LIMIT = 46 << 20
UPDATE_LIMIT = 26 << 20

LOADS = 3
LAGS = (0, 2, 4, 6, 7, 9, 11, 13, 15)
RING = 6
SLOTS = 5
AHEAD = 3


def dot(a, b, ca=1, cb=0):
    return lax.dot_general(a, b, (((ca,), (cb,)), ((), ())), preferred_element_type=F32)


def gelu(half):
    t = jnp.tanh(half * (H0 + H1 * (half * half)))
    return half + half * t


def gelu_both(half):
    sq = half * half
    t = jnp.tanh(half * (H0 + H1 * sq))
    s = 1.0 + t
    u = half * s
    return u, s + u * (1.0 - t) * (H0 + (3.0 * H1) * sq)


def layer_forward(h_ref, w1b_ref, w2b_ref, u_ref, hs_ref, chunk, tile):
    rows, width = h_ref.shape[0], w1b_ref.shape[1]
    for r in range(0, rows, chunk):
        hb = h_ref[r:r + chunk, :].astype(BF16)
        if hs_ref is not None:
            hs_ref[r:r + chunk, :] = hb
        for n in range(0, width, tile):
            u_ref[r:r + chunk, n:n + tile] = gelu(dot(hb, w1b_ref[:, n:n + tile])).astype(BF16)
        h_ref[r:r + chunk, :] = h_ref[r:r + chunk, :] + dot(u_ref[r:r + chunk, :], w2b_ref[...])


def update_kernel(rate, x_ref, y_ref, w1_hbm, w2_hbm, m1_hbm, m2_hbm, gr_ref,
                  w1o_hbm, w2o_hbm, m1o_hbm, m2o_hbm, loss_ref, h_ref,
                  w1_ref, w2_ref, m1_ref, m2_ref, w1b_ref, w2b_ref, u_ref, in_sem, out_sem):
    layers, width = w1_hbm.shape[0], w1_hbm.shape[1]
    states = ((w1_hbm, w1_ref, w1o_hbm), (w2_hbm, w2_ref, w2o_hbm), (m1_hbm, m1_ref, m1o_hbm), (m2_hbm, m2_ref, m2o_hbm))

    def reads(layer):
        slot = layer % SLOTS
        pairs = [(src, buf) for src, buf, _ in states]
        return [pltpu.make_async_copy(src.at[layer], buf.at[slot], in_sem.at[slot, n]) for n, (src, buf) in enumerate(pairs)]

    def writes(layer):
        slot = layer % SLOTS
        return [pltpu.make_async_copy(buf.at[slot], dst.at[layer], out_sem.at[slot, n])
                for n, (_, buf, dst) in enumerate(states)]

    for layer in range(AHEAD):
        for copy in reads(layer):
            copy.start()
    h_ref[...] = x_ref[...].astype(F32)

    @pl.loop(0, layers)
    def _(layer):
        slot = layer % SLOTS

        @pl.when(layer + AHEAD < layers)
        def _():
            @pl.when(layer + AHEAD >= SLOTS)
            def _():
                for copy in writes(layer + AHEAD - SLOTS):
                    copy.wait()
            for copy in reads(layer + AHEAD):
                copy.start()

        for copy in reads(layer):
            copy.wait()
        mom = MOMENTUM * m1_ref[slot] + gr_ref[layer, :width, :].astype(F32)
        m1_ref[slot] = mom
        new = w1_ref[slot] - rate * mom
        w1_ref[slot] = new
        w1b_ref[...] = (0.5 * new).astype(BF16)
        for n in range(0, w2_ref.shape[1], width):
            part = slice(n, n + width)
            mom = MOMENTUM * m2_ref[slot, part, :] + gr_ref[layer, width:, part].astype(F32)
            m2_ref[slot, part, :] = mom
            new = w2_ref[slot, part, :] - rate * mom
            w2_ref[slot, part, :] = new
            w2b_ref[part, :] = new.astype(BF16)
        for copy in writes(layer):
            copy.start(priority=1)
        layer_forward(h_ref, w1b_ref, w2b_ref, u_ref, None, 512, 256)

    resid = h_ref[...] - y_ref[...].astype(F32)
    loss_ref[...] = jnp.sum((resid * resid).T, axis=0, keepdims=True) / (2 * width)
    for layer in range(layers - SLOTS, layers):
        for copy in writes(layer):
            copy.wait()


def gradient_kernel(scale, x_ref, y_ref, w1f_hbm, w2f_hbm, sum_ref, w1_hbm, w2_hbm, hs_hbm,
                    w1f_buf, w2f_buf, w1_buf, w2_buf, hs_buf, load_sem, save_sem, in_sem, g_ref, gb_ref, gt_ref, ht_ref, u_ref, q_ref,
                    grad_ref, r0_ref, r1_ref, r2_ref, r3_ref, send_sem, recv_sem):
    layers = w1f_hbm.shape[0]
    pod, data = lax.axis_index("pod"), lax.axis_index("data")
    z, y, x, c = pod // 2, pod % 2, data // 2, data % 2
    places = (x, y, z)
    neighbours = ((pod, (1 - x) * 2 + c), (z * 2 + (1 - y), data), ((1 - z) * 2 + y, data))
    sibling = (pod, x * 2 + (1 - c))
    rows, width = g_ref.shape
    hidden = u_ref.shape[1]
    block = 2 * width
    recv_refs = (r0_ref, r1_ref, r2_ref, r3_ref)
    third = hidden // 128 * 3 // 8 * 128
    parts = ((0, third), (third, third), (2 * third, hidden - 2 * third))

    saved = ((w1_hbm, w1_buf), (w2_hbm, w2_buf), (hs_hbm, hs_buf))

    def loads(layer):
        slot = layer % LOADS
        return [pltpu.make_async_copy(src.at[layer], buf.at[slot], load_sem.at[slot, n])
                for n, (src, buf) in enumerate(((w1f_hbm, w1f_buf), (w2f_hbm, w2f_buf)))]

    def saves(layer):
        slot = layer % 2
        return [pltpu.make_async_copy(buf.at[slot], dst.at[layer], save_sem.at[slot, n]) for n, (dst, buf) in enumerate(saved)]

    def reads(layer):
        slot = layer % 2
        return [pltpu.make_async_copy(src.at[layer], buf.at[slot], in_sem.at[slot, n]) for n, (src, buf) in enumerate(saved)]

    for layer in range(LOADS - 1):
        for copy in loads(layer):
            copy.start()
    barrier = pltpu.get_barrier_semaphore()
    for peer in neighbours + (sibling,):
        pl.semaphore_signal(barrier, inc=1, device_id=peer, device_id_type=MESH)
    g_ref[...] = x_ref[...].astype(F32)

    @pl.loop(0, layers)
    def _(layer):
        slot = layer % 2

        @pl.when(layer + LOADS - 1 < layers)
        def _():
            for copy in loads(layer + LOADS - 1):
                copy.start()

        @pl.when(layer >= 2)
        def _():
            for copy in saves(layer - 2):
                copy.wait()

        for copy in loads(layer):
            copy.wait()
        w1_buf[slot] = (0.5 * w1f_buf[layer % LOADS]).astype(BF16)
        w2_buf[slot] = w2f_buf[layer % LOADS].astype(BF16)
        layer_forward(g_ref, w1_buf.at[slot], w2_buf.at[slot], u_ref, hs_buf.at[slot], 1024, 256)

        @pl.when(layer < layers - 2)
        def _():
            for copy in saves(layer):
                copy.start()

    g_ref[...] = (g_ref[...] - y_ref[...].astype(F32)) * scale
    pl.semaphore_wait(barrier, 4)

    def ring(slot):
        return slot % RING

    def context(slot):
        if isinstance(slot, int):
            turn = [(slot + k) % 3 for k in range(3)]
            return slot, slot % RING, [places[k] for k in turn], [neighbours[k] for k in turn]
        start = slot % 3
        first = ((2 - start) * (1 - start) // 2, start * (2 - start), start * (start - 1) // 2)
        turned = [[sum(first[b] * values[(b + k) % 3] for b in range(3)) for k in range(3)]
                  for values in (places, [n[0] for n in neighbours], [n[1] for n in neighbours])]
        return slot, slot % RING, turned[0], list(zip(turned[1], turned[2]))

    def region(ctx, part, stage):
        return sum([ctx[2][(part + n - 1) % 3] * (block >> (n + 1)) for n in range(1, stage + 1)], c * (block // 2))

    def message(ctx, m, part):
        slot, kept, bits, peers = ctx
        if m in (0, 7):
            stage, size, cols, peer = 0, block // 2, slice(None), sibling
            mine, other = c * size, (1 - c) * size
        else:
            stage = m if m <= 3 else 7 - m
            size, cols = block >> (stage + 1), pl.ds(*parts[part])
            axis = (part + stage - 1) % 3
            base, peer = region(ctx, part, stage - 1), peers[axis]
            mine, other = base + bits[axis] * size, base + (1 - bits[axis]) * size
        if m <= 3:
            src = grad_ref.at[kept, pl.ds(pl.multiple_of(other, 16), size), cols]
            dst = recv_refs[stage].at[slot, :, cols]
        else:
            src = sum_ref.at[slot, pl.ds(pl.multiple_of(mine, 16), size), cols]
            dst = src
        return pltpu.make_async_remote_copy(
            src_ref=src, dst_ref=dst, send_sem=send_sem.at[slot, m, part], recv_sem=recv_sem.at[slot, m, part],
            device_id=peer, device_id_type=MESH)

    def parts_of(m):
        return (0,) if m in (0, 7) else (0, 1, 2)

    def accumulate(ctx, stage, part):
        slot, kept = ctx[:2]
        size = block >> (stage + 1)
        if stage == 0:
            mine, cols = c * size, pl.ds(0, hidden)
        else:
            mine, cols = region(ctx, part, stage), pl.ds(*parts[part])
        where = pl.ds(pl.multiple_of(mine, 16), size)
        total = grad_ref[kept, where, cols].astype(F32) + recv_refs[stage][slot, :, cols].astype(F32)
        if stage == 3:
            sum_ref[slot, where, cols] = total.astype(BF16)
        else:
            grad_ref[kept, where, cols] = total.astype(BF16)

    def step(s, slot):
        ctx = context(slot)
        if s > 0:
            m = s - 1
            for part in parts_of(m):
                message(ctx, m, part).wait()
                if m <= 3:
                    accumulate(ctx, m, part)
                if m not in (0, 7) and s < 8 and s != 7:
                    message(ctx, s, part).start()
        if s == 0 or s == 1 or s == 7:
            for part in parts_of(s):
                message(ctx, s, part).start()

    def comm_point(it, parity):
        for s in reversed(range(9)):
            if LAGS[s] % 2 == parity:
                done = it - 1 - (LAGS[s] - parity) // 2

                @pl.when(done >= 0)
                def _():
                    step(s, layers - 1 - done)

    tile, chunk = 256, 256

    @pl.loop(0, layers)
    def _(it):
        comm_point(it, 0)

        layer = layers - 1 - it

        @pl.when((it >= 1) & (it + 1 < layers))
        def _():
            for copy in reads(layer - 1):
                copy.start()

        @pl.when(it >= 2)
        def _():
            for copy in reads(layer):
                copy.wait()

        w1_ref, w2_ref, hs_ref = (buf.at[layer % 2] for buf in (w1_buf, w2_buf, hs_buf))

        gb_ref[...] = g_ref[...].astype(BF16)
        gt_ref[...] = gb_ref[...].T
        ht_ref[...] = hs_ref[...].T

        def first(n, r):
            cols = slice(n, n + tile)
            a = dot(hs_ref[r:r + chunk, :], w1_ref[:, cols])
            gu = dot(gb_ref[r:r + chunk, :], w2_ref[cols, :], 1, 1)
            u, slope = gelu_both(a)
            u_ref[r:r + chunk, cols] = u.astype(BF16)
            q_ref[r:r + chunk, cols] = (slope * gu).astype(BF16)

        def carry(n, r):
            cols = slice(n, n + tile)
            g_ref[r:r + chunk, :] = g_ref[r:r + chunk, :] + dot(q_ref[r:r + chunk, cols], w1_ref[:, cols], 1, 1)

        def grad_second(n):
            cols = slice(n, n + tile)
            grad_ref[ring(layer), width:, cols] = (2.0 * dot(gt_ref[...], u_ref[:, cols])).astype(BF16).T

        def grad_first(n):
            cols = slice(n, n + tile)
            grad_ref[ring(layer), :width, cols] = dot(ht_ref[...], q_ref[:, cols]).astype(BF16)

        def tile_step(n, previous):
            for i, r in enumerate(range(0, rows, chunk)):
                if previous is not None:
                    carry(previous, r)
                    if i == rows // chunk // 2 - 1:
                        grad_second(previous)
                if n is not None:
                    first(n, r)
            if previous is not None:
                grad_first(previous)

        tiles = list(range(0, hidden, tile)) + [None]
        for i, n in enumerate(tiles):
            if i == len(tiles) // 2:
                comm_point(it, 1)
            tile_step(n, tiles[i - 1] if i > 0 else None)

    taken = [sum(2 * n + 2 + lag < 2 * layers for lag in LAGS) for n in range(layers)]
    while min(taken) < 9:
        for n in reversed(range(layers)):
            if taken[n] < 9:
                step(taken[n], layers - 1 - n)
                taken[n] += 1


def solution(mesh):
    n_pod = mesh.shape['pod']
    n_data = mesh.shape['data']
    rows_spec = P(('pod', 'data'), None)
    full_spec = P()

    def train_step(w_first, w_second, m_first, m_second, x_now, y_now, x_next, y_next):
        layers, width, hidden = w_first.shape
        rows = x_now.shape[0]
        batch = rows * n_pod * n_data
        shape = jax.ShapeDtypeStruct
        matmul_flops = 2 * rows * width * hidden * layers

        grads = pl.pallas_call(
            functools.partial(gradient_kernel, 0.5 / (batch * width)),
            in_specs=[pl.BlockSpec(memory_space=pltpu.VMEM)] * 2 + [pl.BlockSpec(memory_space=pl.ANY)] * 2,
            out_specs=[pl.BlockSpec(memory_space=pltpu.VMEM)] + [pl.BlockSpec(memory_space=pl.ANY)] * 3,
            out_shape=[pltpu.VMEM((layers, 2 * width, hidden), BF16), shape((layers - 2, width, hidden), BF16),
                       shape((layers - 2, hidden, width), BF16), shape((layers - 2, rows, width), BF16)],
            scratch_shapes=[
                pltpu.VMEM((LOADS, width, hidden), F32),
                pltpu.VMEM((LOADS, hidden, width), F32),
                pltpu.VMEM((2, width, hidden), BF16),
                pltpu.VMEM((2, hidden, width), BF16),
                pltpu.VMEM((2, rows, width), BF16),
                pltpu.SemaphoreType.DMA((LOADS, 2)),
                pltpu.SemaphoreType.DMA((2, 3)),
                pltpu.SemaphoreType.DMA((2, 3)),
                pltpu.VMEM((rows, width), F32),
                pltpu.VMEM((rows, width), BF16),
                pltpu.VMEM((width, rows), BF16),
                pltpu.VMEM((width, rows), BF16),
                pltpu.VMEM((rows, hidden), BF16),
                pltpu.VMEM((rows, hidden), BF16),
                pltpu.VMEM((RING, 2 * width, hidden), BF16),
                pltpu.VMEM((layers, width, hidden), BF16),
                pltpu.VMEM((layers, width // 2, hidden), BF16),
                pltpu.VMEM((layers, width // 4, hidden), BF16),
                pltpu.VMEM((layers, width // 8, hidden), BF16),
                pltpu.SemaphoreType.DMA((layers, 8, 3)),
                pltpu.SemaphoreType.DMA((layers, 8, 3)),
            ],
            compiler_params=pltpu.CompilerParams(vmem_limit_bytes=BACK_LIMIT,
                                                 collective_id=0, has_side_effects=True),
            cost_estimate=pl.CostEstimate(flops=7 * matmul_flops, bytes_accessed=80_000_000, transcendentals=0),
            name="gradient",
        )(x_now, y_now, w_first, w_second)[0]

        outs = pl.pallas_call(
            functools.partial(update_kernel, LEARN_BASE / layers),
            in_specs=[pl.BlockSpec(memory_space=pltpu.VMEM)] * 2 + [pl.BlockSpec(memory_space=pl.ANY)] * 4 +
                     [pl.BlockSpec(memory_space=pltpu.VMEM)],
            out_specs=[pl.BlockSpec(memory_space=pl.ANY)] * 4 + [pl.BlockSpec(memory_space=pltpu.VMEM)] * 2,
            out_shape=[shape((layers, width, hidden), F32), shape((layers, hidden, width), F32),
                       shape((layers, width, hidden), F32), shape((layers, hidden, width), F32),
                       shape((1, rows), F32), shape((rows, width), F32)],
            scratch_shapes=[pltpu.VMEM((SLOTS, width, hidden), F32), pltpu.VMEM((SLOTS, hidden, width), F32),
                            pltpu.VMEM((SLOTS, width, hidden), F32), pltpu.VMEM((SLOTS, hidden, width), F32),
                            pltpu.VMEM((width, hidden), BF16), pltpu.VMEM((hidden, width), BF16),
                            pltpu.VMEM((rows, hidden), BF16),
                            pltpu.SemaphoreType.DMA((SLOTS, 4)), pltpu.SemaphoreType.DMA((SLOTS, 4))],
            compiler_params=pltpu.CompilerParams(vmem_limit_bytes=UPDATE_LIMIT),
            cost_estimate=pl.CostEstimate(flops=2 * matmul_flops, bytes_accessed=160_000_000, transcendentals=0),
            name="update_forward_next",
        )(x_next, y_next, w_first, w_second, m_first, m_second, pltpu.with_memory_space_constraint(grads, pltpu.VMEM))
        return outs[0], outs[1], outs[2], outs[3], outs[4].reshape(rows), outs[5]

    return jax.shard_map(train_step, mesh=mesh,
                         in_specs=(full_spec,) * 4 + (rows_spec,) * 4,
                         out_specs=(full_spec,) * 4 + (P(('pod', 'data')), rows_spec),
                         check_vma=False)
```
